32 devices in a mesh: gx: 4 (over x, core), gy: 2 (over y), gz: 4 (over z).
Axes of the slice: x: 2, y: 2, z: 4, core: 2. Of those that a mesh axis runs over, the one named last changes fastest.
Arguments:
- start_field: float32 [256, 128, 1024], P('gx', 'gy', 'gz'), may hold values from -6 to 6
- right_side: float32 [256, 128, 1024], P('gx', 'gy', 'gz'), may hold values from -6 to 6
Outputs:
- corrected: float32 [256, 128, 1024], P('gx', 'gy', 'gz')
The draws below stay inside these ranges and needn't reach their ends.
All inputs are finite; a program needn't handle non-finite values.
Results may differ from the reference program's by a relative error of at most 0.00002.
Values sent between devices are 32-bit elements; how exact they have to be, the bound alone decides.
A program may use at most 128 MiB of HBM per device.

```python
import jax
import jax.numpy as jnp
from jax import lax

FINE_SWEEPS = 2
COARSE_SWEEPS = 4
NX = 256
NY = 128
NZ = 1024


def draw_right_side(key, part):
    noise_field = jnp.clip(jax.random.normal(key, (NX, NY, NZ), jnp.float32), -6.0, 6.0)
    return noise_field


def levels(stream_key, dims, shards, smallest, top_value):
    def one(position, shards_of):
        draws = jax.random.uniform(jax.random.fold_in(jax.random.fold_in(stream_key, 6), position), (shards_of,), jnp.float32, smallest / len(shards), top_value / len(shards))
        return jnp.repeat(jnp.exp(draws), dims[position] // shards_of).reshape((-1,) + (1,) * (len(dims) - position - 1))

    factor_of = one(*shards[0])
    for cut in shards[1:]:
        factor_of = factor_of * one(*cut)
    return factor_of


def bell_draw(key, shape, spread, reach, pieces=(), kind=jnp.bfloat16):
    drawn = jax.random.normal(key, shape, jnp.float32) * spread
    if len(pieces) > 0:
        drawn = levels(key, shape, pieces, -0.22, 0.18) * drawn
    return jnp.clip(drawn, min=-reach, max=reach).astype(kind)


def setup_inputs(seed: int = 0) -> dict:
    seeds = jax.random.split(jax.random.key(seed), 3)
    start_field = bell_draw(seeds[0], (NX, NY, NZ), 1.0, 6.0, ((0, 4), (1, 2), (2, 4)), jnp.float32)
    right_side = draw_right_side(jax.random.fold_in(seeds[2], 71), 0)
    return {"start_field": start_field, "right_side": right_side}


relaxation = 6.0 / 7.0


def apply_stencil(values):
    padded = jnp.pad(values, 1)
    beside = padded[2:, 1:-1, 1:-1] + padded[:-2, 1:-1, 1:-1]
    beside = beside + padded[1:-1, 2:, 1:-1] + padded[1:-1, :-2, 1:-1]
    beside = beside + padded[1:-1, 1:-1, 2:] + padded[1:-1, 1:-1, :-2]
    return 6.0 * values - beside


def restrict_axis(values, which_axis):
    length = values.shape[which_axis]
    half_len = length // 2
    even_rows = lax.slice_in_dim(values, 0, length, 2, which_axis)
    odd_rows = lax.slice_in_dim(values, 1, length, 2, which_axis)
    zero_row = jnp.zeros_like(lax.slice_in_dim(even_rows, 0, 1, 1, which_axis))
    following = jnp.concatenate([lax.slice_in_dim(even_rows, 1, half_len, 1, which_axis), zero_row], which_axis)
    return 0.25 * even_rows + 0.5 * odd_rows + 0.25 * following


def prolong_axis(values, which_axis):
    length = values.shape[which_axis]
    zero_row = jnp.zeros_like(lax.slice_in_dim(values, 0, 1, 1, which_axis))
    previous = jnp.concatenate([zero_row, lax.slice_in_dim(values, 0, length - 1, 1, which_axis)], which_axis)
    even_rows = 0.5 * (previous + values)
    paired = jnp.stack([even_rows, values], which_axis + 1)
    new_shape = list(values.shape)
    new_shape[which_axis] = 2 * length
    return jnp.reshape(paired, new_shape)


def reference(start_field, right_side):
    smoothed = start_field
    for sweep_num in range(FINE_SWEEPS):
        smoothed = smoothed + (relaxation / 6.0) * (right_side - apply_stencil(smoothed))
    residual = right_side - apply_stencil(smoothed)
    coarse_rhs = restrict_axis(restrict_axis(restrict_axis(residual, 0), 1), 2)
    correction = jnp.zeros_like(coarse_rhs)
    for sweep_num in range(COARSE_SWEEPS):
        correction = correction + (relaxation / 1.5) * (coarse_rhs - 0.25 * apply_stencil(correction))
    fine_corr = prolong_axis(prolong_axis(prolong_axis(correction, 0), 1), 2)
    return smoothed + fine_corr
```

```python
import functools

import jax
import jax.numpy as jnp
from jax import lax
from jax.experimental import pallas as pl
from jax.experimental.pallas import tpu as pltpu
from jax.sharding import PartitionSpec as P

OMEGA = 6.0 / 7.0
SMOOTH = 1.0 - OMEGA
STEP = OMEGA / 1.5
COARSE_SWEEPS = 4
LANES = 128
PAD = 8
FX = 4
FINE_SLOT = 8
COARSE_SLOT = 16
SR = 12
AXES = ("gx", "gy", "gz")
MESH = pl.DeviceIdType.MESH
SIDES = (-1, 0, 1)
NEIGHBOURS = tuple((x, y, z) for x in SIDES for y in SIDES for z in SIDES if (x, y, z) != (0, 0, 0))
PLANAR = tuple(d for d in NEIGHBOURS if d[2] == 0)
SPILL_Z = tuple(d for d in NEIGHBOURS if d[2] and not (d[0] and d[1]))
N_COPIES = len(NEIGHBOURS) + 2 * len(PLANAR) + len(SPILL_Z)


def rotated(values, shift):
    return pltpu.roll(values, shift % LANES if isinstance(shift, int) else shift, values.ndim - 1)


def split_dot(values, matrix):
    high = values.astype(jnp.bfloat16)
    rest = values - high.astype(jnp.float32)
    middle = rest.astype(jnp.bfloat16)
    low = (rest - middle.astype(jnp.float32)).astype(jnp.bfloat16)
    total = jnp.dot(low, matrix, preferred_element_type=jnp.float32)
    total = total + jnp.dot(middle, matrix, preferred_element_type=jnp.float32)
    return total + jnp.dot(high, matrix, preferred_element_type=jnp.float32)


def fine_block(ny):
    rows = ny + PAD
    return 24 if rows % 24 == 0 else 8


def correct_kernel(
    sizes, start_hbm, right_hbm, u2, q_ref,
    u0, u1, f, px, py, e0, e1, e2, s1, s2, rs, sp, spr, fm,
    ys, yr, xr, xe, xer,
    mp, pk, em, kc, rm, rp, rpx, c0, c1, c2, c3, d0, d1, d2, d3, g0, g1, g2, ad,
    local_sem, send_sem, recv_sem,
):
    nt, nxp, nyp, _ = f.shape
    nx, ny = nxp - 2 * FX, nyp - 2 * PAD
    nz = nt * LANES
    mx, my, mz = nx // 2, ny // 2, nz // 2
    tiles = fm.shape[0]
    wide = ny + PAD
    block = fine_block(ny)
    blocks = range(0, wide, block)
    rows_c = my + PAD
    me = tuple(lax.axis_index(a) for a in AXES)
    f32 = jnp.float32

    def there(d):
        found = None
        for at, step, size in zip(me, d, sizes):
            if step:
                one = at < size - 1 if step > 0 else at > 0
                found = one if found is None else jnp.logical_and(found, one)
        return found

    def minus(d):
        return tuple(-c for c in d)

    def device(d):
        return tuple(at + step for at, step in zip(me, d))

    sent = []

    def send(src, dst, d):
        number = len(sent)

        def copy(to):
            return pltpu.make_async_remote_copy(
                src_ref=src, dst_ref=dst, send_sem=send_sem.at[number],
                recv_sem=recv_sem.at[number], device_id=device(to), device_id_type=MESH)

        @pl.when(there(d))
        def _():
            copy(d).start()

        sent.append((copy, d, dst))
        return number

    def arrive(number):
        copy, d, dst = sent[number]

        @pl.when(there(minus(d)))
        def _():
            copy(minus(d)).wait_recv()

        @pl.when(jnp.logical_not(there(minus(d))))
        def _():
            dst[...] = jnp.zeros(dst.shape, dst.dtype)

    def iota(shape, axis):
        return lax.broadcasted_iota(jnp.int32, shape, axis)

    chunks = 4 if nx % 4 == 0 else 1
    per = nx // chunks
    loads = []
    for c in range(chunks):
        for into, source in ((u0, start_hbm), (f, right_hbm)):
            for t in range(nt):
                load = pltpu.make_async_copy(
                    source.at[pl.ds(c * per, per), :, pl.ds(t * LANES, LANES)],
                    into.at[t, pl.ds(FX + c * per, per), pl.ds(PAD, ny), :], local_sem.at[len(loads)])
                load.start()
                loads.append(load)

    barrier = pltpu.get_barrier_semaphore()
    expected = jnp.int32(0)
    for d in NEIGHBOURS:
        @pl.when(there(d))
        def _(d=d):
            pl.semaphore_signal(barrier, inc=1, device_id=device(d), device_id_type=MESH)
        expected = expected + there(d).astype(jnp.int32)

    def ones(flag):
        return jnp.where(flag, 1.0, 0.0).astype(f32)

    below = tuple(ones(at > 0) for at in me)
    above = tuple(ones(at < size - 1) for at, size in zip(me, sizes))

    def inside(index, axis, length):
        return jnp.where(index < 0, below[axis], jnp.where(index >= length, above[axis], 1.0))

    edge = jnp.zeros((PAD, LANES), f32)

    def clear_rows(x, _):
        for ref in (u0, u1, u2, f):
            for t in range(nt):
                ref[t, x, 0:PAD, :] = edge
                ref[t, x, PAD + ny:, :] = edge
        return 0

    lax.fori_loop(0, nxp, clear_rows, 0)
    for ref, planes in ((u0, (-2, -1, nx, nx + 1)), (u1, (-3, -2, nx + 1, nx + 2)),
                        (u2, (-4, -3, nx + 2, nx + 3)), (f, (-3, -2, -1, nx, nx + 1, nx + 2))):
        for x in planes:
            for t in range(nt):
                ref[t, x + FX] = jnp.zeros((nyp, LANES), f32)

    def clear_px(i, _):
        for t in range(nt):
            px[t, i, 0:PAD, :] = edge
            px[t, i, PAD + ny:, :] = jnp.zeros((2 * PAD, LANES), f32)
        return 0

    lax.fori_loop(0, mx + 4, clear_px, 0)
    for ref in (e0, e1, e2):
        ref[...] = jnp.zeros(ref.shape, f32)
    for ref in (s1, s2, rs):
        for g in range(tiles):
            ref[g, 0:PAD, :] = edge
            ref[g, PAD + wide:, :] = edge
    pk[...] = jnp.zeros(pk.shape, f32)
    for ref in (c0, c1, c2, c3):
        def clear_c(i, _, ref=ref):
            ref[i, 0:PAD, :] = edge
            ref[i, PAD + rows_c:, :] = edge
            return 0
        lax.fori_loop(0, mx + PAD, clear_c, 0)
    for ref in (d0, d1, d2, d3):
        for g in range(tiles):
            ref[g, 0:PAD, :] = edge
            ref[g, PAD + rows_c:, :] = edge
    for ref in (g0, g1, g2):
        ref[...] = jnp.zeros(ref.shape, f32)
    xe[...] = jnp.zeros(xe.shape, f32)

    lane1 = iota((1, LANES), 1)

    def slots(lane, width):
        return lax.rem(lane + width // 2, LANES) // width, lax.rem(lane + width // 2, width) - width // 2

    def zinside(o, reach_low, reach_high):
        low = jnp.logical_and(o >= 0, o < reach_low)
        high = jnp.logical_and(o < 0, o >= -reach_high)
        return jnp.where(low, below[2], jnp.where(high, above[2], 0.0))

    for g in range(tiles):
        shape = (wide, LANES)
        p, o = slots(iota(shape, 1), FINE_SLOT)
        value = inside(g * 16 + p - 8, 0, nx) * inside(iota(shape, 0) - 4, 1, ny)
        fm[g] = value * zinside(o, 3, 3)
        shape = (rows_c, LANES)
        p, o = slots(iota(shape, 1), COARSE_SLOT)
        value = inside(g * 8 + p - 4, 0, mx) * inside(iota(shape, 0) - 4, 1, my)
        em[g] = value * zinside(o, 4, 3)
    kc[...] = inside(iota((rows_c, LANES), 0) - 4, 1, my)

    lane = iota((block, LANES), 1)
    slot, _ = slots(lane, FINE_SLOT)
    first_lane, last_lane = lane == 0, lane == LANES - 1
    low_half = lane < LANES // 2
    inject_1 = jnp.where(low_half, below[2], above[2]) * SMOOTH

    def row_mask(at):
        index = iota((block, LANES), 0) + (at - 4)
        if at == 0 or at + block == wide:
            return inside(index, 1, ny)
        return None

    row_masks = [row_mask(at) for at in blocks]

    def plane_mask(X):
        return inside(X - FX, 0, nx)

    def near(u, X, at, middle, before_x, after_x, inject):
        sums = []
        row = at + 4
        left = [rotated(p, 1) for p in middle]
        right = [rotated(p, LANES - 1) for p in middle]
        for t in range(nt):
            before = jnp.where(first_lane, left[t - 1] if t else inject, left[t])
            after = jnp.where(last_lane, right[t + 1] if t < nt - 1 else inject, right[t])
            total = before_x[t] + after_x[t]
            total = total + (u[t, X, pl.ds(row - 1, block), :] + u[t, X, pl.ds(row + 1, block), :])
            sums.append(total + (before + after))
        return sums

    def plane_of(u, X, at):
        return [u[t, X, pl.ds(at + 4, block), :] for t in range(nt)]

    def edges_of(planes):
        return jnp.where(low_half, planes[0], planes[nt - 1])

    def place(X):
        index = X + (8 - FX)
        return lax.div(index, 16), lax.rem(index, 16)

    def keep_edges(ref, X, at, planes):
        g, p = place(X)
        pltpu.store(
            ref.at[g, pl.ds(PAD + at, block), :], rotated(edges_of(planes), p * FINE_SLOT), mask=slot == p)

    def sweep(old, new, X0, X1, inject_of, keeps):
        for at, mask in zip(blocks, row_masks):
            def step(X, carry, at=at, mask=mask):
                before_x, middle = carry
                after_x = plane_of(old, X + 1, at)
                sums = near(old, X, at, middle, before_x, after_x, inject_of(X, at))
                factor = SMOOTH * plane_mask(X)
                if mask is not None:
                    factor = factor * mask
                results = []
                for t in range(nt):
                    value = (middle[t] + f[t, X, pl.ds(at + 4, block), :] + sums[t]) * factor
                    new[t, X, pl.ds(at + 4, block), :] = value
                    results.append(value)
                keeps(X, at, middle, results)
                return middle, after_x

            lax.fori_loop(X0, X1, step, (plane_of(old, X0 - 1, at), plane_of(old, X0, at)))

    def keeps_1(X, at, middle, results):
        keep_edges(e0, X, at, middle)
        keep_edges(e1, X, at, results)

    zero_b = jnp.zeros((block, LANES), f32)
    for c in range(chunks):
        for load in loads[c * 2 * nt:(c + 1) * 2 * nt]:
            load.wait()
        first = FX - 1 if c == 0 else FX + c * per - 1
        last = FX + nx + 1 if c == chunks - 1 else FX + (c + 1) * per - 1
        sweep(u0, u1, first, last, lambda X, at: zero_b, keeps_1)

    pl.semaphore_wait(barrier, expected)

    def inject_2(X, at):
        return edges_of(plane_of(u0, X, at)) * inject_1

    sweep(u1, u2, FX - 2, FX + nx + 2, inject_2, lambda X, at, middle, results: keep_edges(e2, X, at, results))

    def sides(ref, g, rows, width, slot_s, off, edge_ref):
        here = ref[g, rows, :]
        count = LANES // width
        zero = jnp.zeros_like(here)
        previous = rotated(ref[g - 1, rows, :], width) if g else zero
        following = rotated(ref[g + 1, rows, :], LANES - width) if g < tiles - 1 else zero
        total = jnp.where(slot_s == 0, previous, rotated(here, width))
        total = total + jnp.where(slot_s == count - 1, following, rotated(here, LANES - width))
        start, length = rows.start, rows.size
        total = total + ref[g, pl.ds(start - 1, length), :] + ref[g, pl.ds(start + 1, length), :]
        touching = edge_ref[g, rows, :]
        total = total + jnp.where(off == 0, touching, rotated(here, 1))
        total = total + jnp.where(off == -1, touching, rotated(here, LANES - 1))
        return here, total

    lane_w = iota((wide, LANES), 1)
    slot_w, off_w = slots(lane_w, FINE_SLOT)
    rows_w = pl.ds(PAD, wide)
    at_edge = jnp.where(jnp.logical_or(off_w == 0, off_w == -1), SMOOTH, 0.0)
    for g in range(tiles):
        s1[g, rows_w, :] = e0[g, rows_w, :] * fm[g] * at_edge
    for g in range(tiles):
        here, total = sides(s1, g, rows_w, FINE_SLOT, slot_w, off_w, e1)
        s2[g, rows_w, :] = (here + total) * fm[g] * SMOOTH

    for g in range(tiles):
        here = s2[g, rows_w, :]
        value = jnp.where(off_w == 0, rotated(here, 1), jnp.where(off_w == 1, rotated(here, 3), 0.0))
        value = jnp.where(off_w == -1, rotated(here, LANES - 1), value)
        sp[g, rows_w, :] = jnp.where(off_w == -2, rotated(here, LANES - 3), value)
    flat = u2.reshape(nt, nxp * nyp, LANES)

    def rows_along(y):
        return pl.ds(FX * nyp + PAD + y, nx, stride=nyp)

    for side, y in ((0, -2), (1, ny)):
        for k in range(2):
            for t in range(nt):
                ys[side, k, t] = flat[t, rows_along(y + k), :]
    corners = [d for d in PLANAR if d[0] and d[1]]
    for n, (dx, dy, _) in enumerate(corners):
        X, y = (FX + nx if dx > 0 else FX - 1), (PAD + ny if dy > 0 else PAD - 1)
        for t in range(nt):
            xe[n, t:t + 1, :] = u2[t, X, y:y + 1, :]

    def row_part(d, first, length):
        if d == 0:
            return pl.ds(first, length)
        return pl.ds(first + (length - PAD if d > 0 else 0), PAD)

    def tile_part(d):
        if d == 0:
            return pl.ds(0, tiles)
        return pl.ds(tiles - 1 if d > 0 else 0, 1)

    spill_sent = []
    for n, dx in enumerate((-1, 1)):
        source = u2.at[:, pl.ds(FX + nx if dx > 0 else FX - 2, 2), pl.ds(PAD, ny), :]
        spill_sent.append(send(source, xr.at[n], (dx, 0, 0)))
    for n, dy in enumerate((-1, 1)):
        spill_sent.append(send(ys.at[n], yr.at[n], (0, dy, 0)))
    for n, d in enumerate(corners):
        spill_sent.append(send(xe.at[n], xer.at[n], d))
    for n, (dx, dy, dz) in enumerate(SPILL_Z):
        tp, rpart = tile_part(dx), row_part(dy, 8, wide)
        source = sp.at[tp, rpart, :]
        spill_sent.append(send(source, spr.at[n, pl.ds(0, tp.size), pl.ds(0, rpart.size), :], (dx, dy, dz)))

    def residual(X, at, mask, middle, before_x, after_x):
        g, p = place(X)
        inject = rotated(s2[g, pl.ds(PAD + at, block), :], lax.rem(LANES - p * FINE_SLOT, LANES))
        sums = near(u2, X, at, middle, before_x, after_x, inject)
        factor = plane_mask(X)
        if mask is not None:
            factor = factor * mask
        return [(f[t, X, pl.ds(at + 4, block), :] - 6.0 * middle[t] + sums[t]) * factor for t in range(nt)]

    for at, mask in zip(blocks, row_masks):
        def step_x(i, carry, at=at, mask=mask):
            before_x, middle, part = carry
            X = FX + 2 * i - 3
            after_x = plane_of(u2, X + 1, at)
            beyond = plane_of(u2, X + 2, at)
            odd = residual(X, at, mask, middle, before_x, after_x)
            even = residual(X + 1, at, mask, after_x, middle, beyond)
            quarter = [0.25 * e for e in even]
            for t in range(nt):
                px[t, i, pl.ds(at + 4, block), :] = part[t] + 0.5 * odd[t] + quarter[t]
            return after_x, beyond, quarter

        start = (plane_of(u2, FX - 4, at), plane_of(u2, FX - 3, at), [zero_b] * nt)
        _, _, part = lax.fori_loop(0, mx + 3, step_x, start)
        for t in range(nt):
            px[t, mx + 3, pl.ds(at + 4, block), :] = part[t]

    for g in range(tiles):
        here, total = sides(s2, g, rows_w, FINE_SLOT, slot_w, off_w, e2)
        rs[g, rows_w, :] = (total - 6.0 * here) * fm[g]

    quarter, half = 0.25 * STEP, 0.5 * STEP

    def step_y(i, _):
        for t in range(nt):
            evens = px[t, i, pl.ds(0, rows_c, stride=2), :]
            odds = px[t, i, pl.ds(1, rows_c, stride=2), :]
            nexts = px[t, i, pl.ds(2, rows_c, stride=2), :]
            py[i, :, t * LANES:(t + 1) * LANES] = quarter * (evens + nexts) + half * odds
        return 0

    lax.fori_loop(0, mx + 4, step_y, 0)

    def weights(gap, scale):
        outer = jnp.logical_or(gap == 0, gap == 2)
        return jnp.where(gap == 1, 0.5 * scale, jnp.where(outer, 0.25 * scale, 0.0))

    def packed_index(o):
        k = jnp.where(o >= 4, mz + 3 - o, jnp.where(o >= 2, mz - 2 + o, jnp.where(o >= 0, -1 - o, mz - 1 - o)))
        return jnp.where(o <= -7, o + 6, jnp.where(jnp.logical_and(o <= -4, o >= -6), -4 - o, k))

    z_of, n_of = iota((nz, LANES), 0), iota((nz, LANES), 1)
    down = weights(z_of - 2 * n_of, 1.0)
    q_of, o_of = slots(n_of, COARSE_SLOT)
    pack_down = jnp.where(jnp.logical_and(q_of == 0, o_of != -3), weights(z_of - 2 * packed_index(o_of), 1.0), 0.0)
    down = jnp.concatenate([down, pack_down], 1).astype(jnp.bfloat16)
    k_of, n_of = iota((2 * LANES, LANES), 0), iota((2 * LANES, LANES), 1)
    over = k_of >= LANES
    p_of, of_of = slots(jnp.where(over, k_of - LANES, k_of), FINE_SLOT)
    p_of = jnp.where(over, p_of + 16, p_of)
    zf_of = jnp.where(of_of >= 0, -1 - of_of, nz - 1 - of_of)
    q_of, o_of = slots(n_of, COARSE_SLOT)
    kk_of = jnp.where(o_of == -3, mz - 1, packed_index(o_of))
    used = jnp.logical_and(of_of != 3, of_of != -4)
    pack_strip = weights(p_of - 2 * q_of, 1.0) * weights(zf_of - 2 * kk_of, 1.0)
    pack_strip = jnp.where(used, pack_strip, 0.0).astype(jnp.bfloat16)

    group = 4 if (mx + 4) % 4 == 0 else 1
    lane_c = iota((rows_c, LANES), 1)
    slot_c, off_c = slots(lane_c, COARSE_SLOT)
    rows_m = pl.ds(PAD, rows_c)

    def place_c(index):
        return lax.div(index, 8), lax.rem(index, 8)

    def step_z(j, _):
        both = split_dot(py[pl.ds(j * group, group)].reshape(group * rows_c, nz), down)
        both = both.reshape(group, rows_c, 2 * LANES)
        for n in range(group):
            index = j * group + n + 2
            mp[index, rows_m, :] = both[n, :, :LANES]
            g, q = place_c(index)
            pltpu.store(pk.at[g, rows_m, :], rotated(both[n, :, LANES:], q * COARSE_SLOT), mask=slot_c == q)
        return 0

    lax.fori_loop(0, (mx + 4) // group, step_z, 0)

    def strip_y(g):
        start = SR - 8
        evens = rs[g, pl.ds(start, rows_c, stride=2), :]
        odds = rs[g, pl.ds(start + 1, rows_c, stride=2), :]
        nexts = rs[g, pl.ds(start + 2, rows_c, stride=2), :]
        return quarter * (evens + nexts) + half * odds

    parts = [strip_y(g) for g in range(tiles)] + [jnp.zeros((rows_c, LANES), f32)]
    for g in range(tiles):
        pk[g, rows_m, :] += split_dot(jnp.concatenate(parts[g:g + 2], 1), pack_strip)

    def plane_part(dx):
        if dx == 0:
            return pl.ds(2, mx + 4)
        return pl.ds(mx, 6) if dx > 0 else pl.ds(2, 5)

    waits_m, waits_p = {}, {}
    for n, d in enumerate(PLANAR):
        planes, rows = plane_part(d[0]), row_part(d[1], PAD, rows_c)
        target = rm.at[n, pl.ds(0, planes.size), pl.ds(0, rows.size), :]
        waits_m[d] = send(mp.at[planes, rows, :], target, d)
    for n, d in enumerate(NEIGHBOURS):
        tp, rows = tile_part(d[0]), row_part(d[1], PAD, rows_c)
        if d[0] == 0:
            target = rp.at[(d[1] + 1) * 3 + d[2] + 1, :, pl.ds(0, rows.size), :]
        else:
            target = rpx.at[n, :, pl.ds(0, rows.size), :]
        waits_p[d] = send(pk.at[tp, rows, :], target, d)

    for number in spill_sent:
        arrive(number)
    lane_n = iota((ny, LANES), 1)
    _, off_n = slots(lane_n, FINE_SLOT)
    for n, X in enumerate((FX + nx - 2, FX)):
        for k in range(2):
            for t in range(nt):
                u2[t, X + k, pl.ds(PAD, ny), :] += xr[n, t, k]
    for n, y in enumerate((ny - 2, 0)):
        for k in range(2):
            for t in range(nt):
                flat[t, rows_along(y + k), :] += yr[n, k, t]
    for n, (dx, dy, _) in enumerate(corners):
        X, y = (FX if dx > 0 else FX + nx - 1), (PAD if dy > 0 else PAD + ny - 1)
        for t in range(nt):
            u2[t, X, y:y + 1, :] += xer[n, t:t + 1, :]
    at_z = {d: n for n, d in enumerate(SPILL_Z)}
    sums = {}
    for dz in (-1, 1):
        main = at_z[(0, 0, dz)]
        for dx in (-1, 1):
            spr[main, tiles - 1 if dx < 0 else 0] += spr[at_z[(dx, 0, dz)], 0]
        for dy in (-1, 1):
            row = 0 if dy > 0 else wide - PAD
            for g in range(tiles):
                spr[main, g, row:row + PAD] += spr[at_z[(0, dy, dz)], g, 0:PAD]
    for g in range(tiles):
        sp_off = off_w >= 0
        s1[g, rows_w, :] = jnp.where(sp_off, spr[at_z[(0, 0, 1)], g], spr[at_z[(0, 0, -1)], g])
    low_lanes, high_lanes = lane_n < 2, lane_n >= LANES - 2

    def add_z(x, _):
        g, p = place(x + FX)
        value = rotated(s1[g, pl.ds(SR, ny), :], lax.rem(LANES - p * FINE_SLOT, LANES))
        u2[0, x + FX, pl.ds(PAD, ny), :] += jnp.where(low_lanes, value, 0.0)
        u2[nt - 1, x + FX, pl.ds(PAD, ny), :] += jnp.where(high_lanes, value, 0.0)
        return 0

    lax.fori_loop(0, nx, add_z, 0)

    for d in PLANAR:
        arrive(waits_m[d])
    for d in NEIGHBOURS:
        arrive(waits_p[d])
    at_p = {d: n for n, d in enumerate(NEIGHBOURS)}
    at_m = {d: n for n, d in enumerate(PLANAR)}
    last = rows_c - PAD

    def row_at(dy):
        return 0 if dy > 0 else last

    pieces = {}
    for dz in SIDES:
        for g in range(tiles):
            base = pk[g, rows_m, :] if dz == 0 else rp[3 + dz + 1, g]
            pieces[dz, g] = [base[r:r + PAD] for r in range(0, rows_c, PAD)]
            for dy in (-1, 1):
                extra = rp[(dy + 1) * 3 + dz + 1, g, 0:PAD]
                pieces[dz, g][row_at(dy) // PAD] += extra
        for dx in (-1, 1):
            g = 0 if dx > 0 else tiles - 1
            for dy in SIDES:
                ref = rpx.at[at_p[(dx, dy, dz)], 0]
                if dy == 0:
                    for n in range(rows_c // PAD):
                        pieces[dz, g][n] += ref[n * PAD:(n + 1) * PAD]
                else:
                    pieces[dz, g][row_at(dy) // PAD] += ref[0:PAD]
    for g in range(tiles):
        own, low, high = (jnp.concatenate(pieces[dz, g], 0) for dz in (0, 1, -1))
        value = jnp.where(jnp.logical_and(off_c >= -2, off_c <= 1), own, 0.0)
        value = value + jnp.where(off_c >= 0, rotated(low, LANES - 4), rotated(high, 3))
        d0[g, rows_m, :] = value * em[g]
        lowest = jnp.where(jnp.logical_or(off_c == 0, off_c == 1), rotated(low, LANES - 2), 0.0)
        highest = jnp.where(jnp.logical_or(off_c == -1, off_c == -2), rotated(high, 6), 0.0)
        ad[g] = lowest + highest + jnp.where(off_c == -1, rotated(own, 2), 0.0)

    first_c, last_c = lane_c == 0, lane_c == LANES - 1
    near_c = jnp.logical_or(lane_c < 2, lane_c >= LANES - 2)

    def plane_mask_c(index):
        return inside(index - 4, 0, mx)

    def build(index, extra=None):
        g, q = place_c(index)
        here = mp[index, rows_m, :] if extra is None else extra
        value = here + jnp.where(near_c, rotated(ad[g], lax.rem(LANES - q * COARSE_SLOT, LANES)), 0.0)
        value = value * (kc[...] * plane_mask_c(index))
        c0[index, rows_m, :] = value
        pltpu.store(g0.at[g, rows_m, :], rotated(value, q * COARSE_SLOT), mask=slot_c == q)

    def rows_added(index):
        first = mp[index, pl.ds(PAD, PAD), :] + rm[at_m[(0, 1, 0)], index - 2, 0:PAD]
        middle = mp[index, pl.ds(2 * PAD, rows_c - 2 * PAD), :]
        final = mp[index, pl.ds(PAD + last, PAD), :] + rm[at_m[(0, -1, 0)], index - 2, 0:PAD]
        return jnp.concatenate([first, middle, final], 0)

    def planes_added(dx, k, own):
        value = rm[at_m[(dx, 0, 0)], k] + (own if own is not None else 0.0)
        first = value[0:PAD] + rm[at_m[(dx, 1, 0)], k, 0:PAD]
        final = value[last:] + rm[at_m[(dx, -1, 0)], k, 0:PAD]
        return jnp.concatenate([first, value[PAD:last], final], 0)

    for k in range(6):
        build(k, planes_added(1, k, rows_added(k) if k >= 2 else None))

    def build_inner(index, _):
        build(index, rows_added(index))
        return 0

    lax.fori_loop(6, mx + 2, build_inner, 0)
    for k in range(5):
        index = mx + 2 + k
        build(index, planes_added(-1, k, rows_added(index) if index < mx + 6 else None))

    grids, strips, touch = (c0, c1, c2, c3), (d0, d1, d2, d3), (g0, g1, g2)
    for k in range(COARSE_SWEEPS - 1):
        old, new = grids[k], grids[k + 1]

        def sweep_c(index, _, old=old, new=new, k=k):
            g, q = place_c(index)
            inject = rotated(strips[k][g, rows_m, :], lax.rem(LANES - q * COARSE_SLOT, LANES))
            here = old[index, rows_m, :]
            total = here + old[index - 1, rows_m, :] + old[index + 1, rows_m, :]
            total = total + old[index, pl.ds(PAD - 1, rows_c), :] + old[index, pl.ds(PAD + 1, rows_c), :]
            total = total + jnp.where(first_c, inject, rotated(here, 1))
            total = total + jnp.where(last_c, inject, rotated(here, LANES - 1))
            value = total * (kc[...] * (plane_mask_c(index) * (0.25 * STEP))) + c0[index, rows_m, :]
            new[index, rows_m, :] = value
            if k < COARSE_SWEEPS - 2:
                pltpu.store(touch[k + 1].at[g, rows_m, :], rotated(value, q * COARSE_SLOT), mask=slot_c == q)
            return 0

        lax.fori_loop(k + 1, mx + 6 - k, sweep_c, 0)
        for g in range(tiles):
            here, total = sides(strips[k], g, rows_m, COARSE_SLOT, slot_c, off_c, touch[k])
            strips[k + 1][g, rows_m, :] = (here + total) * (em[g] * (0.25 * STEP)) + d0[g, rows_m, :]

    up = weights(iota((mz, nz), 1) - 2 * iota((mz, nz), 0), 2.0).astype(jnp.bfloat16)
    three = 3 if (mx + 1) % 3 == 0 else 1

    def prolong_z(j, _):
        value = split_dot(c3[pl.ds(3 + j * three, three), rows_m, :].reshape(three * rows_c, LANES), up)
        for n in range(three):
            g, q = place_c(3 + j * three + n)
            outside = 0.5 * rotated(d3[g, rows_m, :], lax.rem(LANES - q * COARSE_SLOT, LANES))
            for t in range(nt):
                part = value[n * rows_c:(n + 1) * rows_c, t * LANES:(t + 1) * LANES]
                if t == 0:
                    part = part + jnp.where(first_c, outside, 0.0)
                q_ref[j * three + n, t] = part
        return 0

    lax.fori_loop(0, (mx + 1) // three, prolong_z, 0)

    for copy, d, _ in sent:
        @pl.when(there(d))
        def _(copy=copy, d=d):
            copy(d).wait_send()


def add_kernel(per, smooth_ref, q_ref, out_hbm, both, out_ref, sems):
    mx, nt, my = q_ref.shape[0] - 1, q_ref.shape[1], q_ref.shape[2] - PAD
    ny = 2 * my

    def spread(p, _):
        for t in range(nt):
            here = q_ref[p, t, 4:4 + my, :]
            before = q_ref[p, t, 3:3 + my, :]
            both[p, t, pl.ds(0, my, stride=2), :] = 0.5 * (before + here)
            both[p, t, pl.ds(1, my, stride=2), :] = here
        return 0

    def add(j, _):
        for t in range(nt):
            part = pl.ds(t * LANES, LANES)
            here = both[j + 1, t]
            first = smooth_ref[t, 2 * j + FX, PAD:PAD + ny, :]
            second = smooth_ref[t, 2 * j + FX + 1, PAD:PAD + ny, :]
            out_ref[2 * j, :, part] = first + 0.5 * (both[j, t] + here)
            out_ref[2 * j + 1, :, part] = second + here
        return 0

    copies = []
    spread(0, 0)
    for c in range(mx // per):
        lax.fori_loop(c * per + 1, (c + 1) * per + 1, spread, 0, unroll=2)
        lax.fori_loop(c * per, (c + 1) * per, add, 0)
        rows = pl.ds(2 * c * per, 2 * per)
        copies.append(pltpu.make_async_copy(out_ref.at[rows], out_hbm.at[rows], sems.at[c]))
        copies[-1].start()
    for copy in copies:
        copy.wait()


def on_device(sizes, start_field, right_side):
    nx, ny, nz = start_field.shape
    nt, mx, my = nz // LANES, nx // 2, ny // 2
    tiles = (nx + 16) // 16
    f32 = jnp.float32

    def vm(*shape):
        return pltpu.VMEM(shape, f32)

    fine_shape = (nt, nx + 2 * FX, ny + 2 * PAD, LANES)
    fine = vm(*fine_shape)
    strip = vm(tiles, ny + 3 * PAD, LANES)
    strip_c = vm(tiles, my + 3 * PAD, LANES)
    coarse = vm(mx + PAD, my + 3 * PAD, LANES)
    vmem = pl.BlockSpec(memory_space=pltpu.VMEM)
    smooth, q = pl.pallas_call(
        functools.partial(correct_kernel, sizes),
        out_shape=(
            pltpu.VMEM(fine_shape, f32),
            pltpu.VMEM((mx + 1, nt, my + PAD, LANES), f32),
        ),
        in_specs=[pl.BlockSpec(memory_space=pltpu.HBM)] * 2,
        out_specs=(vmem, vmem),
        scratch_shapes=[
            fine, fine, fine,
            vm(nt, mx + 4, ny + 3 * PAD, LANES), vm(mx + 4, my + PAD, nz),
            strip, strip, strip, strip, strip, strip,
            strip, vm(len(SPILL_Z), tiles, ny + PAD, LANES), vm(tiles, ny + PAD, LANES),
            vm(2, 2, nt, nx, LANES), vm(2, 2, nt, nx, LANES), vm(2, nt, 2, ny, LANES), vm(4, PAD, LANES), vm(4, PAD, LANES),
            coarse, strip_c, vm(tiles, my + PAD, LANES), vm(my + PAD, LANES),
            vm(len(PLANAR), mx + 4, my + PAD, LANES), vm(9, tiles, my + PAD, LANES),
            vm(len(NEIGHBOURS), 1, my + PAD, LANES),
            coarse, coarse, coarse, coarse, strip_c, strip_c, strip_c, strip_c, strip_c, strip_c, strip_c,
            vm(tiles, my + PAD, LANES),
            pltpu.SemaphoreType.DMA((8 * nt,)),
            pltpu.SemaphoreType.DMA((N_COPIES,)),
            pltpu.SemaphoreType.DMA((N_COPIES,)),
        ],
        compiler_params=pltpu.CompilerParams(
            collective_id=0, has_side_effects=True, vmem_limit_bytes=48 * 1024 * 1024),
    )(*(pltpu.with_memory_space_constraint(a, pltpu.HBM) for a in (start_field, right_side)))
    per = 8 if mx % 8 == 0 else 1
    return pl.pallas_call(
        functools.partial(add_kernel, per),
        out_shape=jax.ShapeDtypeStruct((nx, ny, nz), f32),
        in_specs=[vmem, vmem],
        out_specs=pl.BlockSpec(memory_space=pl.ANY),
        scratch_shapes=[
            pltpu.VMEM((mx + 1, nt, ny, LANES), f32), pltpu.VMEM((nx, ny, nz), f32),
            pltpu.SemaphoreType.DMA((mx // per,)),
        ],
        compiler_params=pltpu.CompilerParams(vmem_limit_bytes=24 * 1024 * 1024),
    )(smooth, q)


def solution(mesh):
    placed = (P(*AXES), P(*AXES))
    sizes = tuple(mesh.shape[a] for a in AXES)
    return jax.shard_map(
        functools.partial(on_device, sizes), mesh=mesh, in_specs=placed, out_specs=P(*AXES), check_vma=False
    )
```

```python
import functools

import jax
import jax.numpy as jnp
from jax import lax
from jax.experimental import pallas as pl
from jax.experimental.pallas import tpu as pltpu
from jax.sharding import PartitionSpec as P

OMEGA = 6.0 / 7.0
SMOOTH = 1.0 - OMEGA
STEP = OMEGA / 1.5
COARSE_SWEEPS = 4
BY = 8
BYX = 5
BYC = 12
BYZ = 8
LANES = 128
PAD = 8
FX = 4
FINE_SLOT = 8
COARSE_SLOT = 16
SR = 12
AXES = ("gx", "gy", "gz")
MESH = pl.DeviceIdType.MESH
SIDES = (-1, 0, 1)
NEIGHBOURS = tuple((x, y, z) for x in SIDES for y in SIDES for z in SIDES if (x, y, z) != (0, 0, 0))
PLANAR = tuple(d for d in NEIGHBOURS if d[2] == 0)
SPILL_Z = tuple(d for d in NEIGHBOURS if d[2] and not (d[0] and d[1]))
N_COPIES = len(NEIGHBOURS) + 2 * len(PLANAR) + len(SPILL_Z)


def rotated(values, shift):
    return pltpu.roll(values, shift % LANES if isinstance(shift, int) else shift, values.ndim - 1)


def split_dot(values, matrix):
    high = values.astype(jnp.bfloat16)
    rest = values - high.astype(jnp.float32)
    middle = rest.astype(jnp.bfloat16)
    low = (rest - middle.astype(jnp.float32)).astype(jnp.bfloat16)
    total = jnp.dot(low, matrix, preferred_element_type=jnp.float32)
    total = total + jnp.dot(middle, matrix, preferred_element_type=jnp.float32)
    return total + jnp.dot(high, matrix, preferred_element_type=jnp.float32)


def unrolled(first, last, body, carry, by):
    count = (last - first) // by

    def several(j, carry):
        for n in range(by):
            carry = body(first + j * by + n, carry)
        return carry

    carry = lax.fori_loop(0, count, several, carry)
    for index in range(first + count * by, last):
        carry = body(index, carry)
    return carry


def fine_block(ny):
    rows = ny + PAD
    return 24 if rows % 24 == 0 else 8


def correct_kernel(
    sizes, start_hbm, right_hbm, u2, q_ref,
    u0, u1, f, px, py, e0, e1, e2, s1, s2, rs, sp, spr, fm,
    ys, yr, xr, xe, xer,
    mp, pk, em, kc, rm, rp, rpx, c0, c1, c2, c3, d0, d1, d2, d3, g0, g1, g2, ad,
    local_sem, send_sem, recv_sem,
):
    nt, nxp, nyp, _ = f.shape
    nx, ny = nxp - 2 * FX, nyp - 2 * PAD
    nz = nt * LANES
    mx, my, mz = nx // 2, ny // 2, nz // 2
    tiles = fm.shape[0]
    wide = ny + PAD
    block = fine_block(ny)
    blocks = range(0, wide, block)
    rows_c = my + PAD
    me = tuple(lax.axis_index(a) for a in AXES)
    f32 = jnp.float32

    def there(d):
        found = None
        for at, step, size in zip(me, d, sizes):
            if step:
                one = at < size - 1 if step > 0 else at > 0
                found = one if found is None else jnp.logical_and(found, one)
        return found

    def minus(d):
        return tuple(-c for c in d)

    def device(d):
        return tuple(at + step for at, step in zip(me, d))

    sent = []

    def send(src, dst, d):
        number = len(sent)

        def copy(to):
            return pltpu.make_async_remote_copy(
                src_ref=src, dst_ref=dst, send_sem=send_sem.at[number],
                recv_sem=recv_sem.at[number], device_id=device(to), device_id_type=MESH)

        @pl.when(there(d))
        def _():
            copy(d).start()

        sent.append((copy, d, dst))
        return number

    def arrive(number):
        copy, d, dst = sent[number]

        @pl.when(there(minus(d)))
        def _():
            copy(minus(d)).wait_recv()

        @pl.when(jnp.logical_not(there(minus(d))))
        def _():
            dst[...] = jnp.zeros(dst.shape, dst.dtype)

    def iota(shape, axis):
        return lax.broadcasted_iota(jnp.int32, shape, axis)

    chunks = 4 if nx % 4 == 0 else 1
    per = nx // chunks
    loads = []
    for c in range(chunks):
        for into, source in ((u0, start_hbm), (f, right_hbm)):
            for t in range(nt):
                load = pltpu.make_async_copy(
                    source.at[pl.ds(c * per, per), :, pl.ds(t * LANES, LANES)],
                    into.at[t, pl.ds(FX + c * per, per), pl.ds(PAD, ny), :], local_sem.at[len(loads)])
                load.start()
                loads.append(load)

    barrier = pltpu.get_barrier_semaphore()
    expected = jnp.int32(0)
    for d in NEIGHBOURS:
        @pl.when(there(d))
        def _(d=d):
            pl.semaphore_signal(barrier, inc=1, device_id=device(d), device_id_type=MESH)
        expected = expected + there(d).astype(jnp.int32)

    def ones(flag):
        return jnp.where(flag, 1.0, 0.0).astype(f32)

    below = tuple(ones(at > 0) for at in me)
    above = tuple(ones(at < size - 1) for at, size in zip(me, sizes))

    def inside(index, axis, length):
        return jnp.where(index < 0, below[axis], jnp.where(index >= length, above[axis], 1.0))

    edge = jnp.zeros((PAD, LANES), f32)

    def clear_rows(x, _):
        for ref in (u0, u1, u2, f):
            for t in range(nt):
                ref[t, x, 0:PAD, :] = edge
                ref[t, x, PAD + ny:, :] = edge
        return 0

    lax.fori_loop(0, nxp, clear_rows, 0)
    for ref, planes in ((u0, (-2, -1, nx, nx + 1)), (u1, (-3, -2, nx + 1, nx + 2)),
                        (u2, (-4, -3, nx + 2, nx + 3)), (f, (-3, -2, -1, nx, nx + 1, nx + 2))):
        for x in planes:
            for t in range(nt):
                ref[t, x + FX] = jnp.zeros((nyp, LANES), f32)

    def clear_px(i, _):
        for t in range(nt):
            px[t, i, 0:PAD, :] = edge
            px[t, i, PAD + ny:, :] = jnp.zeros((2 * PAD, LANES), f32)
        return 0

    lax.fori_loop(0, mx + 4, clear_px, 0)
    for ref in (e0, e1, e2):
        ref[...] = jnp.zeros(ref.shape, f32)
    for ref in (s1, s2, rs):
        for g in range(tiles):
            ref[g, 0:PAD, :] = edge
            ref[g, PAD + wide:, :] = edge
    pk[...] = jnp.zeros(pk.shape, f32)
    for ref in (c0, c1, c2, c3):
        def clear_c(i, _, ref=ref):
            ref[i, 0:PAD, :] = edge
            ref[i, PAD + rows_c:, :] = edge
            return 0
        lax.fori_loop(0, mx + PAD, clear_c, 0)
    for ref in (d0, d1, d2, d3):
        for g in range(tiles):
            ref[g, 0:PAD, :] = edge
            ref[g, PAD + rows_c:, :] = edge
    for ref in (g0, g1, g2):
        ref[...] = jnp.zeros(ref.shape, f32)
    xe[...] = jnp.zeros(xe.shape, f32)

    lane1 = iota((1, LANES), 1)

    def slots(lane, width):
        return lax.rem(lane + width // 2, LANES) // width, lax.rem(lane + width // 2, width) - width // 2

    def zinside(o, reach_low, reach_high):
        low = jnp.logical_and(o >= 0, o < reach_low)
        high = jnp.logical_and(o < 0, o >= -reach_high)
        return jnp.where(low, below[2], jnp.where(high, above[2], 0.0))

    for g in range(tiles):
        shape = (wide, LANES)
        p, o = slots(iota(shape, 1), FINE_SLOT)
        value = inside(g * 16 + p - 8, 0, nx) * inside(iota(shape, 0) - 4, 1, ny)
        fm[g] = value * zinside(o, 3, 3)
        shape = (rows_c, LANES)
        p, o = slots(iota(shape, 1), COARSE_SLOT)
        value = inside(g * 8 + p - 4, 0, mx) * inside(iota(shape, 0) - 4, 1, my)
        em[g] = value * zinside(o, 4, 3)
    kc[...] = inside(iota((rows_c, LANES), 0) - 4, 1, my)

    lane = iota((block, LANES), 1)
    slot, _ = slots(lane, FINE_SLOT)
    first_lane, last_lane = lane == 0, lane == LANES - 1
    low_half = lane < LANES // 2
    inject_1 = jnp.where(low_half, below[2], above[2]) * SMOOTH

    def row_mask(at):
        index = iota((block, LANES), 0) + (at - 4)
        if at == 0 or at + block == wide:
            return inside(index, 1, ny)
        return None

    row_masks = [row_mask(at) for at in blocks]

    def plane_mask(X):
        return inside(X - FX, 0, nx)

    def near(u, X, at, middle, before_x, after_x, inject):
        sums = []
        row = at + 4
        left = [rotated(p, 1) for p in middle]
        right = [rotated(p, LANES - 1) for p in middle]
        for t in range(nt):
            before = jnp.where(first_lane, left[t - 1] if t else inject, left[t])
            after = jnp.where(last_lane, right[t + 1] if t < nt - 1 else inject, right[t])
            total = before_x[t] + after_x[t]
            total = total + (u[t, X, pl.ds(row - 1, block), :] + u[t, X, pl.ds(row + 1, block), :])
            sums.append(total + (before + after))
        return sums

    def plane_of(u, X, at):
        return [u[t, X, pl.ds(at + 4, block), :] for t in range(nt)]

    def edges_of(planes):
        return jnp.where(low_half, planes[0], planes[nt - 1])

    def place(X):
        index = X + (8 - FX)
        return lax.div(index, 16), lax.rem(index, 16)

    def keep_edges(ref, X, at, planes):
        g, p = place(X)
        pltpu.store(
            ref.at[g, pl.ds(PAD + at, block), :], rotated(edges_of(planes), p * FINE_SLOT), mask=slot == p)

    def sweep(old, new, X0, X1, inject_of, keeps):
        for at, mask in zip(blocks, row_masks):
            def step(X, carry, at=at, mask=mask):
                before_x, middle = carry
                after_x = plane_of(old, X + 1, at)
                sums = near(old, X, at, middle, before_x, after_x, inject_of(X, at))
                factor = SMOOTH * plane_mask(X)
                if mask is not None:
                    factor = factor * mask
                for t in range(nt):
                    value = (middle[t] + f[t, X, pl.ds(at + 4, block), :] + sums[t]) * factor
                    new[t, X, pl.ds(at + 4, block), :] = value
                keeps(X, at, middle)
                return middle, after_x

            unrolled(X0, X1, step, (plane_of(old, X0 - 1, at), plane_of(old, X0, at)), BY)

    def keeps_1(X, at, middle):
        keep_edges(e0, X, at, middle)

    zero_b = jnp.zeros((block, LANES), f32)
    for c in range(chunks):
        for load in loads[c * 2 * nt:(c + 1) * 2 * nt]:
            load.wait()
        first = FX - 1 if c == 0 else FX + c * per - 1
        last = FX + nx + 1 if c == chunks - 1 else FX + (c + 1) * per - 1
        sweep(u0, u1, first, last, lambda X, at: zero_b, keeps_1)

    pl.semaphore_wait(barrier, expected)

    def inject_2(X, at):
        return edges_of(plane_of(u0, X, at)) * inject_1

    sweep(u1, u2, FX - 2, FX + nx + 2, inject_2, lambda X, at, middle: keep_edges(e1, X, at, middle))

    def sides(ref, g, rows, width, slot_s, off, edge_ref):
        here = ref[g, rows, :]
        count = LANES // width
        zero = jnp.zeros_like(here)
        previous = rotated(ref[g - 1, rows, :], width) if g else zero
        following = rotated(ref[g + 1, rows, :], LANES - width) if g < tiles - 1 else zero
        total = jnp.where(slot_s == 0, previous, rotated(here, width))
        total = total + jnp.where(slot_s == count - 1, following, rotated(here, LANES - width))
        start, length = rows.start, rows.size
        total = total + ref[g, pl.ds(start - 1, length), :] + ref[g, pl.ds(start + 1, length), :]
        touching = edge_ref[g, rows, :]
        total = total + jnp.where(off == 0, touching, rotated(here, 1))
        total = total + jnp.where(off == -1, touching, rotated(here, LANES - 1))
        return here, total

    lane_w = iota((wide, LANES), 1)
    slot_w, off_w = slots(lane_w, FINE_SLOT)
    rows_w = pl.ds(PAD, wide)
    at_edge = jnp.where(jnp.logical_or(off_w == 0, off_w == -1), SMOOTH, 0.0)
    for g in range(tiles):
        s1[g, rows_w, :] = e0[g, rows_w, :] * fm[g] * at_edge
    for g in range(tiles):
        here, total = sides(s1, g, rows_w, FINE_SLOT, slot_w, off_w, e1)
        s2[g, rows_w, :] = (here + total) * fm[g] * SMOOTH

    for g in range(tiles):
        here = s2[g, rows_w, :]
        value = jnp.where(off_w == 0, rotated(here, 1), jnp.where(off_w == 1, rotated(here, 3), 0.0))
        value = jnp.where(off_w == -1, rotated(here, LANES - 1), value)
        sp[g, rows_w, :] = jnp.where(off_w == -2, rotated(here, LANES - 3), value)
    flat = u2.reshape(nt, nxp * nyp, LANES)

    def rows_along(y):
        return pl.ds(FX * nyp + PAD + y, nx, stride=nyp)

    for side, y in ((0, -2), (1, ny)):
        for k in range(2):
            for t in range(nt):
                ys[side, k, t] = flat[t, rows_along(y + k), :]
    corners = [d for d in PLANAR if d[0] and d[1]]
    for n, (dx, dy, _) in enumerate(corners):
        X, y = (FX + nx if dx > 0 else FX - 1), (PAD + ny if dy > 0 else PAD - 1)
        for t in range(nt):
            xe[n, t:t + 1, :] = u2[t, X, y:y + 1, :]

    def row_part(d, first, length):
        if d == 0:
            return pl.ds(first, length)
        return pl.ds(first + (length - PAD if d > 0 else 0), PAD)

    def tile_part(d):
        if d == 0:
            return pl.ds(0, tiles)
        return pl.ds(tiles - 1 if d > 0 else 0, 1)

    spill_sent = []
    for n, dx in enumerate((-1, 1)):
        source = u2.at[:, pl.ds(FX + nx if dx > 0 else FX - 2, 2), pl.ds(PAD, ny), :]
        spill_sent.append(send(source, xr.at[n], (dx, 0, 0)))
    for n, dy in enumerate((-1, 1)):
        spill_sent.append(send(ys.at[n], yr.at[n], (0, dy, 0)))
    for n, d in enumerate(corners):
        spill_sent.append(send(xe.at[n], xer.at[n], d))
    for n, (dx, dy, dz) in enumerate(SPILL_Z):
        tp, rpart = tile_part(dx), row_part(dy, 8, wide)
        source = sp.at[tp, rpart, :]
        spill_sent.append(send(source, spr.at[n, pl.ds(0, tp.size), pl.ds(0, rpart.size), :], (dx, dy, dz)))

    def residual(X, at, mask, middle, before_x, after_x):
        g, p = place(X)
        inject = rotated(s2[g, pl.ds(PAD + at, block), :], lax.rem(LANES - p * FINE_SLOT, LANES))
        keep_edges(e2, X, at, middle)
        sums = near(u2, X, at, middle, before_x, after_x, inject)
        factor = plane_mask(X)
        if mask is not None:
            factor = factor * mask
        return [(f[t, X, pl.ds(at + 4, block), :] - 6.0 * middle[t] + sums[t]) * factor for t in range(nt)]

    for at, mask in zip(blocks, row_masks):
        def step_x(i, carry, at=at, mask=mask):
            before_x, middle, part = carry
            X = FX + 2 * i - 3
            after_x = plane_of(u2, X + 1, at)
            beyond = plane_of(u2, X + 2, at)
            odd = residual(X, at, mask, middle, before_x, after_x)
            even = residual(X + 1, at, mask, after_x, middle, beyond)
            quarter = [0.25 * e for e in even]
            for t in range(nt):
                px[t, i, pl.ds(at + 4, block), :] = part[t] + 0.5 * odd[t] + quarter[t]
            return after_x, beyond, quarter

        start = (plane_of(u2, FX - 4, at), plane_of(u2, FX - 3, at), [zero_b] * nt)
        _, _, part = unrolled(0, mx + 3, step_x, start, BYX)
        for t in range(nt):
            px[t, mx + 3, pl.ds(at + 4, block), :] = part[t]

    for g in range(tiles):
        here, total = sides(s2, g, rows_w, FINE_SLOT, slot_w, off_w, e2)
        rs[g, rows_w, :] = (total - 6.0 * here) * fm[g]

    quarter, half = 0.25 * STEP, 0.5 * STEP

    def step_y(i, _):
        for t in range(nt):
            evens = px[t, i, pl.ds(0, rows_c, stride=2), :]
            odds = px[t, i, pl.ds(1, rows_c, stride=2), :]
            nexts = px[t, i, pl.ds(2, rows_c, stride=2), :]
            py[i, :, t * LANES:(t + 1) * LANES] = quarter * (evens + nexts) + half * odds
        return 0

    unrolled(0, mx + 4, step_y, 0, 4)

    def weights(gap, scale):
        outer = jnp.logical_or(gap == 0, gap == 2)
        return jnp.where(gap == 1, 0.5 * scale, jnp.where(outer, 0.25 * scale, 0.0))

    def packed_index(o):
        k = jnp.where(o >= 4, mz + 3 - o, jnp.where(o >= 2, mz - 2 + o, jnp.where(o >= 0, -1 - o, mz - 1 - o)))
        return jnp.where(o <= -7, o + 6, jnp.where(jnp.logical_and(o <= -4, o >= -6), -4 - o, k))

    z_of, n_of = iota((nz, LANES), 0), iota((nz, LANES), 1)
    down = weights(z_of - 2 * n_of, 1.0)
    q_of, o_of = slots(n_of, COARSE_SLOT)
    pack_down = jnp.where(jnp.logical_and(q_of == 0, o_of != -3), weights(z_of - 2 * packed_index(o_of), 1.0), 0.0)
    down = jnp.concatenate([down, pack_down], 1).astype(jnp.bfloat16)
    k_of, n_of = iota((2 * LANES, LANES), 0), iota((2 * LANES, LANES), 1)
    over = k_of >= LANES
    p_of, of_of = slots(jnp.where(over, k_of - LANES, k_of), FINE_SLOT)
    p_of = jnp.where(over, p_of + 16, p_of)
    zf_of = jnp.where(of_of >= 0, -1 - of_of, nz - 1 - of_of)
    q_of, o_of = slots(n_of, COARSE_SLOT)
    kk_of = jnp.where(o_of == -3, mz - 1, packed_index(o_of))
    used = jnp.logical_and(of_of != 3, of_of != -4)
    pack_strip = weights(p_of - 2 * q_of, 1.0) * weights(zf_of - 2 * kk_of, 1.0)
    pack_strip = jnp.where(used, pack_strip, 0.0).astype(jnp.bfloat16)

    group = 4 if (mx + 4) % 4 == 0 else 1
    lane_c = iota((rows_c, LANES), 1)
    slot_c, off_c = slots(lane_c, COARSE_SLOT)
    rows_m = pl.ds(PAD, rows_c)

    def place_c(index):
        return lax.div(index, 8), lax.rem(index, 8)

    def step_z(j, _):
        both = split_dot(py[pl.ds(j * group, group)].reshape(group * rows_c, nz), down)
        both = both.reshape(group, rows_c, 2 * LANES)
        for n in range(group):
            index = j * group + n + 2
            mp[index, rows_m, :] = both[n, :, :LANES]
            g, q = place_c(index)
            pltpu.store(pk.at[g, rows_m, :], rotated(both[n, :, LANES:], q * COARSE_SLOT), mask=slot_c == q)
        return 0

    unrolled(0, (mx + 4) // group, step_z, 0, 3)

    def strip_y(g):
        start = SR - 8
        evens = rs[g, pl.ds(start, rows_c, stride=2), :]
        odds = rs[g, pl.ds(start + 1, rows_c, stride=2), :]
        nexts = rs[g, pl.ds(start + 2, rows_c, stride=2), :]
        return quarter * (evens + nexts) + half * odds

    parts = [strip_y(g) for g in range(tiles)] + [jnp.zeros((rows_c, LANES), f32)]
    for g in range(tiles):
        pk[g, rows_m, :] += split_dot(jnp.concatenate(parts[g:g + 2], 1), pack_strip)

    def plane_part(dx):
        if dx == 0:
            return pl.ds(2, mx + 4)
        return pl.ds(mx, 6) if dx > 0 else pl.ds(2, 5)

    waits_m, waits_p = {}, {}
    for n, d in enumerate(PLANAR):
        planes, rows = plane_part(d[0]), row_part(d[1], PAD, rows_c)
        target = rm.at[n, pl.ds(0, planes.size), pl.ds(0, rows.size), :]
        waits_m[d] = send(mp.at[planes, rows, :], target, d)
    for n, d in enumerate(NEIGHBOURS):
        tp, rows = tile_part(d[0]), row_part(d[1], PAD, rows_c)
        if d[0] == 0:
            target = rp.at[(d[1] + 1) * 3 + d[2] + 1, :, pl.ds(0, rows.size), :]
        else:
            target = rpx.at[n, :, pl.ds(0, rows.size), :]
        waits_p[d] = send(pk.at[tp, rows, :], target, d)

    for number in spill_sent:
        arrive(number)
    lane_n = iota((ny, LANES), 1)
    _, off_n = slots(lane_n, FINE_SLOT)
    for n, X in enumerate((FX + nx - 2, FX)):
        for k in range(2):
            for t in range(nt):
                u2[t, X + k, pl.ds(PAD, ny), :] += xr[n, t, k]
    for n, y in enumerate((ny - 2, 0)):
        for k in range(2):
            for t in range(nt):
                flat[t, rows_along(y + k), :] += yr[n, k, t]
    for n, (dx, dy, _) in enumerate(corners):
        X, y = (FX if dx > 0 else FX + nx - 1), (PAD if dy > 0 else PAD + ny - 1)
        for t in range(nt):
            u2[t, X, y:y + 1, :] += xer[n, t:t + 1, :]
    at_z = {d: n for n, d in enumerate(SPILL_Z)}
    sums = {}
    for dz in (-1, 1):
        main = at_z[(0, 0, dz)]
        for dx in (-1, 1):
            spr[main, tiles - 1 if dx < 0 else 0] += spr[at_z[(dx, 0, dz)], 0]
        for dy in (-1, 1):
            row = 0 if dy > 0 else wide - PAD
            for g in range(tiles):
                spr[main, g, row:row + PAD] += spr[at_z[(0, dy, dz)], g, 0:PAD]
    for g in range(tiles):
        sp_off = off_w >= 0
        s1[g, rows_w, :] = jnp.where(sp_off, spr[at_z[(0, 0, 1)], g], spr[at_z[(0, 0, -1)], g])
    low_lanes, high_lanes = lane_n < 2, lane_n >= LANES - 2

    def add_z(x, _):
        g, p = place(x + FX)
        value = rotated(s1[g, pl.ds(SR, ny), :], lax.rem(LANES - p * FINE_SLOT, LANES))
        u2[0, x + FX, pl.ds(PAD, ny), :] += jnp.where(low_lanes, value, 0.0)
        u2[nt - 1, x + FX, pl.ds(PAD, ny), :] += jnp.where(high_lanes, value, 0.0)
        return 0

    unrolled(0, nx, add_z, 0, BYZ)

    for d in PLANAR:
        arrive(waits_m[d])
    for d in NEIGHBOURS:
        arrive(waits_p[d])
    at_p = {d: n for n, d in enumerate(NEIGHBOURS)}
    at_m = {d: n for n, d in enumerate(PLANAR)}
    last = rows_c - PAD

    def row_at(dy):
        return 0 if dy > 0 else last

    pieces = {}
    for dz in SIDES:
        for g in range(tiles):
            base = pk[g, rows_m, :] if dz == 0 else rp[3 + dz + 1, g]
            pieces[dz, g] = [base[r:r + PAD] for r in range(0, rows_c, PAD)]
            for dy in (-1, 1):
                extra = rp[(dy + 1) * 3 + dz + 1, g, 0:PAD]
                pieces[dz, g][row_at(dy) // PAD] += extra
        for dx in (-1, 1):
            g = 0 if dx > 0 else tiles - 1
            for dy in SIDES:
                ref = rpx.at[at_p[(dx, dy, dz)], 0]
                if dy == 0:
                    for n in range(rows_c // PAD):
                        pieces[dz, g][n] += ref[n * PAD:(n + 1) * PAD]
                else:
                    pieces[dz, g][row_at(dy) // PAD] += ref[0:PAD]
    for g in range(tiles):
        own, low, high = (jnp.concatenate(pieces[dz, g], 0) for dz in (0, 1, -1))
        value = jnp.where(jnp.logical_and(off_c >= -2, off_c <= 1), own, 0.0)
        value = value + jnp.where(off_c >= 0, rotated(low, LANES - 4), rotated(high, 3))
        d0[g, rows_m, :] = value * em[g]
        lowest = jnp.where(jnp.logical_or(off_c == 0, off_c == 1), rotated(low, LANES - 2), 0.0)
        highest = jnp.where(jnp.logical_or(off_c == -1, off_c == -2), rotated(high, 6), 0.0)
        ad[g] = lowest + highest + jnp.where(off_c == -1, rotated(own, 2), 0.0)

    first_c, last_c = lane_c == 0, lane_c == LANES - 1
    near_c = jnp.logical_or(lane_c < 2, lane_c >= LANES - 2)

    def plane_mask_c(index):
        return inside(index - 4, 0, mx)

    def build(index, extra=None):
        g, q = place_c(index)
        here = mp[index, rows_m, :] if extra is None else extra
        value = here + jnp.where(near_c, rotated(ad[g], lax.rem(LANES - q * COARSE_SLOT, LANES)), 0.0)
        value = value * (kc[...] * plane_mask_c(index))
        c0[index, rows_m, :] = value

    def rows_added(index):
        first = mp[index, pl.ds(PAD, PAD), :] + rm[at_m[(0, 1, 0)], index - 2, 0:PAD]
        middle = mp[index, pl.ds(2 * PAD, rows_c - 2 * PAD), :]
        final = mp[index, pl.ds(PAD + last, PAD), :] + rm[at_m[(0, -1, 0)], index - 2, 0:PAD]
        return jnp.concatenate([first, middle, final], 0)

    def planes_added(dx, k, own):
        value = rm[at_m[(dx, 0, 0)], k] + (own if own is not None else 0.0)
        first = value[0:PAD] + rm[at_m[(dx, 1, 0)], k, 0:PAD]
        final = value[last:] + rm[at_m[(dx, -1, 0)], k, 0:PAD]
        return jnp.concatenate([first, value[PAD:last], final], 0)

    for k in range(6):
        build(k, planes_added(1, k, rows_added(k) if k >= 2 else None))

    def build_inner(index, _):
        build(index, rows_added(index))
        return 0

    unrolled(6, mx + 2, build_inner, 0, BYC)
    for k in range(5):
        index = mx + 2 + k
        build(index, planes_added(-1, k, rows_added(index) if index < mx + 6 else None))

    grids, strips, touch = (c0, c1, c2, c3), (d0, d1, d2, d3), (g0, g1, g2)
    for k in range(COARSE_SWEEPS - 1):
        old, new = grids[k], grids[k + 1]

        def sweep_c(index, _, old=old, new=new, k=k):
            g, q = place_c(index)
            inject = rotated(strips[k][g, rows_m, :], lax.rem(LANES - q * COARSE_SLOT, LANES))
            here = old[index, rows_m, :]
            total = here + old[index - 1, rows_m, :] + old[index + 1, rows_m, :]
            total = total + old[index, pl.ds(PAD - 1, rows_c), :] + old[index, pl.ds(PAD + 1, rows_c), :]
            total = total + jnp.where(first_c, inject, rotated(here, 1))
            total = total + jnp.where(last_c, inject, rotated(here, LANES - 1))
            value = total * (kc[...] * (plane_mask_c(index) * (0.25 * STEP))) + c0[index, rows_m, :]
            new[index, rows_m, :] = value
            pltpu.store(touch[k].at[g, rows_m, :], rotated(here, q * COARSE_SLOT), mask=slot_c == q)
            return 0

        unrolled(k + 1, mx + 6 - k, sweep_c, 0, BYC)
        for g in range(tiles):
            here, total = sides(strips[k], g, rows_m, COARSE_SLOT, slot_c, off_c, touch[k])
            strips[k + 1][g, rows_m, :] = (here + total) * (em[g] * (0.25 * STEP)) + d0[g, rows_m, :]

    up = weights(iota((mz, nz), 1) - 2 * iota((mz, nz), 0), 2.0).astype(jnp.bfloat16)
    three = 3 if (mx + 1) % 3 == 0 else 1

    def prolong_z(j, _):
        value = split_dot(c3[pl.ds(3 + j * three, three), rows_m, :].reshape(three * rows_c, LANES), up)
        for n in range(three):
            g, q = place_c(3 + j * three + n)
            outside = 0.5 * rotated(d3[g, rows_m, :], lax.rem(LANES - q * COARSE_SLOT, LANES))
            for t in range(nt):
                part = value[n * rows_c:(n + 1) * rows_c, t * LANES:(t + 1) * LANES]
                if t == 0:
                    part = part + jnp.where(first_c, outside, 0.0)
                q_ref[j * three + n, t] = part
        return 0

    unrolled(0, (mx + 1) // three, prolong_z, 0, 3)

    for copy, d, _ in sent:
        @pl.when(there(d))
        def _(copy=copy, d=d):
            copy(d).wait_send()


def add_kernel(per, smooth_ref, q_ref, out_hbm, both, out_ref, sems):
    mx, nt, my = q_ref.shape[0] - 1, q_ref.shape[1], q_ref.shape[2] - PAD
    ny = 2 * my

    def spread(p, _):
        for t in range(nt):
            here = q_ref[p, t, 4:4 + my, :]
            before = q_ref[p, t, 3:3 + my, :]
            both[p, t, pl.ds(0, my, stride=2), :] = 0.5 * (before + here)
            both[p, t, pl.ds(1, my, stride=2), :] = here
        return 0

    def add(j, _):
        for t in range(nt):
            part = pl.ds(t * LANES, LANES)
            here = both[j + 1, t]
            first = smooth_ref[t, 2 * j + FX, PAD:PAD + ny, :]
            second = smooth_ref[t, 2 * j + FX + 1, PAD:PAD + ny, :]
            out_ref[2 * j, :, part] = first + 0.5 * (both[j, t] + here)
            out_ref[2 * j + 1, :, part] = second + here
        return 0

    copies = []
    spread(0, 0)
    for c in range(mx // per):
        lax.fori_loop(c * per + 1, (c + 1) * per + 1, spread, 0, unroll=2)
        lax.fori_loop(c * per, (c + 1) * per, add, 0)
        rows = pl.ds(2 * c * per, 2 * per)
        copies.append(pltpu.make_async_copy(out_ref.at[rows], out_hbm.at[rows], sems.at[c]))
        copies[-1].start()
    for copy in copies:
        copy.wait()


def on_device(sizes, start_field, right_side):
    nx, ny, nz = start_field.shape
    nt, mx, my = nz // LANES, nx // 2, ny // 2
    tiles = (nx + 16) // 16
    f32 = jnp.float32

    def vm(*shape):
        return pltpu.VMEM(shape, f32)

    fine_shape = (nt, nx + 2 * FX, ny + 2 * PAD, LANES)
    fine = vm(*fine_shape)
    strip = vm(tiles, ny + 3 * PAD, LANES)
    strip_c = vm(tiles, my + 3 * PAD, LANES)
    coarse = vm(mx + PAD, my + 3 * PAD, LANES)
    vmem = pl.BlockSpec(memory_space=pltpu.VMEM)
    smooth, q = pl.pallas_call(
        functools.partial(correct_kernel, sizes),
        out_shape=(
            pltpu.VMEM(fine_shape, f32),
            pltpu.VMEM((mx + 1, nt, my + PAD, LANES), f32),
        ),
        in_specs=[pl.BlockSpec(memory_space=pltpu.HBM)] * 2,
        out_specs=(vmem, vmem),
        scratch_shapes=[
            fine, fine, fine,
            vm(nt, mx + 4, ny + 3 * PAD, LANES), vm(mx + 4, my + PAD, nz),
            strip, strip, strip, strip, strip, strip,
            strip, vm(len(SPILL_Z), tiles, ny + PAD, LANES), vm(tiles, ny + PAD, LANES),
            vm(2, 2, nt, nx, LANES), vm(2, 2, nt, nx, LANES), vm(2, nt, 2, ny, LANES), vm(4, PAD, LANES), vm(4, PAD, LANES),
            coarse, strip_c, vm(tiles, my + PAD, LANES), vm(my + PAD, LANES),
            vm(len(PLANAR), mx + 4, my + PAD, LANES), vm(9, tiles, my + PAD, LANES),
            vm(len(NEIGHBOURS), 1, my + PAD, LANES),
            coarse, coarse, coarse, coarse, strip_c, strip_c, strip_c, strip_c, strip_c, strip_c, strip_c,
            vm(tiles, my + PAD, LANES),
            pltpu.SemaphoreType.DMA((8 * nt,)),
            pltpu.SemaphoreType.DMA((N_COPIES,)),
            pltpu.SemaphoreType.DMA((N_COPIES,)),
        ],
        compiler_params=pltpu.CompilerParams(
            collective_id=0, has_side_effects=True, vmem_limit_bytes=48 * 1024 * 1024),
    )(*(pltpu.with_memory_space_constraint(a, pltpu.HBM) for a in (start_field, right_side)))
    per = 8 if mx % 8 == 0 else 1
    return pl.pallas_call(
        functools.partial(add_kernel, per),
        out_shape=jax.ShapeDtypeStruct((nx, ny, nz), f32),
        in_specs=[vmem, vmem],
        out_specs=pl.BlockSpec(memory_space=pl.ANY),
        scratch_shapes=[
            pltpu.VMEM((mx + 1, nt, ny, LANES), f32), pltpu.VMEM((nx, ny, nz), f32),
            pltpu.SemaphoreType.DMA((mx // per,)),
        ],
        compiler_params=pltpu.CompilerParams(vmem_limit_bytes=24 * 1024 * 1024),
    )(smooth, q)


def solution(mesh):
    placed = (P(*AXES), P(*AXES))
    sizes = tuple(mesh.shape[a] for a in AXES)
    return jax.shard_map(
        functools.partial(on_device, sizes), mesh=mesh, in_specs=placed, out_specs=P(*AXES), check_vma=False
    )
```

```python
import functools

import jax
import jax.numpy as jnp
from jax import lax
from jax.experimental import pallas as pl
from jax.experimental.pallas import tpu as pltpu
from jax.sharding import PartitionSpec as P

OMEGA = 6.0 / 7.0
SMOOTH = 1.0 - OMEGA
STEP = OMEGA / 1.5
COARSE_SWEEPS = 4
BY = 20
BYX = 14
BYC = 40
BYP = 3
BYZ = 8
LANES = 128
PAD = 8
FX = 4
FINE_SLOT = 8
COARSE_SLOT = 16
SR = 12
AXES = ("gx", "gy", "gz")
MESH = pl.DeviceIdType.MESH
SIDES = (-1, 0, 1)
NEIGHBOURS = tuple((x, y, z) for x in SIDES for y in SIDES for z in SIDES if (x, y, z) != (0, 0, 0))
PLANAR = tuple(d for d in NEIGHBOURS if d[2] == 0)
SPILL_Z = tuple(d for d in NEIGHBOURS if d[2] and not (d[0] and d[1]))
N_COPIES = 160


def rotated(values, shift):
    if isinstance(shift, int) and shift % LANES == 0:
        return values
    return pltpu.roll(values, shift % LANES if isinstance(shift, int) else shift, values.ndim - 1)


def split_dot(values, matrix):
    high = values.astype(jnp.bfloat16)
    rest = values - high.astype(jnp.float32)
    middle = rest.astype(jnp.bfloat16)
    low = (rest - middle.astype(jnp.float32)).astype(jnp.bfloat16)
    total = jnp.dot(low, matrix, preferred_element_type=jnp.float32)
    total = total + jnp.dot(middle, matrix, preferred_element_type=jnp.float32)
    return total + jnp.dot(high, matrix, preferred_element_type=jnp.float32)


def divide(index, by):
    if isinstance(index, int):
        return divmod(index, by)
    return lax.div(index, by), lax.rem(index, by)


def turned_back(values, shift):
    if isinstance(shift, int):
        return rotated(values, -shift)
    return rotated(values, lax.rem(LANES - shift, LANES))


def unrolled(first, last, body, carry, by):
    count = (last - first) // by

    def several(j, carry):
        for n in range(by):
            carry = body(first + j * by + n, carry)
        return carry

    if count:
        carry = lax.fori_loop(0, count, several, carry)
    for index in range(first + count * by, last):
        carry = body(index, carry)
    return carry


def fine_block(ny):
    rows = ny + PAD
    return 24 if rows % 24 == 0 else 8


def correct_kernel(
    sizes, start_hbm, right_hbm, u2, q_ref,
    u0, u1, f, px, py, e0, e1, e2, s1, s2, rs, sp, spr, fm,
    ys, yr, xr, xe, xer,
    mp, pk, pz, em, kc, rm, rp, rpx, c0, c1, c2, c3, d0, d1, d2, d3, g0, g1, g2, ad,
    local_sem, send_sem, recv_sem,
):
    nt, nxp, nyp, _ = f.shape
    nx, ny = nxp - 2 * FX, nyp - 2 * PAD
    nz = nt * LANES
    mx, my, mz = nx // 2, ny // 2, nz // 2
    tiles = fm.shape[0]
    wide = ny + PAD
    block = fine_block(ny)
    blocks = range(0, wide, block)
    rows_c = my + PAD
    me = tuple(lax.axis_index(a) for a in AXES)
    f32 = jnp.float32

    def there(d):
        found = None
        for at, step, size in zip(me, d, sizes):
            if step:
                one = at < size - 1 if step > 0 else at > 0
                found = one if found is None else jnp.logical_and(found, one)
        return found

    def minus(d):
        return tuple(-c for c in d)

    def device(d):
        return tuple(at + step for at, step in zip(me, d))

    sent = []

    def by_direction(numbers):
        found = {}
        for number in numbers:
            found.setdefault(sent[number][1], []).append(number)
        return found.items()

    def send(src, dst, d):
        number = len(sent)

        def copy(to):
            return pltpu.make_async_remote_copy(
                src_ref=src, dst_ref=dst, send_sem=send_sem.at[number],
                recv_sem=recv_sem.at[number], device_id=device(to), device_id_type=MESH)

        sent.append((copy, d))
        return number

    def start(numbers):
        for d, some in by_direction(numbers):
            @pl.when(there(d))
            def _(d=d, some=some):
                for number in some:
                    sent[number][0](d).start()

    def arrive(numbers):
        for d, some in by_direction(numbers):
            @pl.when(there(minus(d)))
            def _(d=d, some=some):
                for number in some:
                    sent[number][0](minus(d)).wait_recv()

    def iota(shape, axis):
        return lax.broadcasted_iota(jnp.int32, shape, axis)

    chunks = tiles - 1
    bounds = [16 * c for c in range(tiles)]
    loads = []
    for low, high in zip(bounds[:-1], bounds[1:]):
        for into, source in ((u0, start_hbm), (f, right_hbm)):
            for t in range(nt):
                load = pltpu.make_async_copy(
                    source.at[pl.ds(low, high - low), :, pl.ds(t * LANES, LANES)],
                    into.at[t, pl.ds(FX + low, high - low), pl.ds(PAD, ny), :], local_sem.at[len(loads)])
                load.start()
                loads.append(load)

    barrier = pltpu.get_barrier_semaphore()
    expected = jnp.int32(0)
    for d in NEIGHBOURS:
        @pl.when(there(d))
        def _(d=d):
            pl.semaphore_signal(barrier, inc=1, device_id=device(d), device_id_type=MESH)
        expected = expected + there(d).astype(jnp.int32)

    def ones(flag):
        return jnp.where(flag, 1.0, 0.0).astype(f32)

    below = tuple(ones(at > 0) for at in me)
    above = tuple(ones(at < size - 1) for at, size in zip(me, sizes))

    def inside(index, axis, length):
        if isinstance(index, int):
            return below[axis] if index < 0 else above[axis] if index >= length else 1.0
        return jnp.where(index < 0, below[axis], jnp.where(index >= length, above[axis], 1.0))

    edge = jnp.zeros((PAD, LANES), f32)

    def clear_rows(x, _):
        for ref in (u0, u1, u2, f):
            for t in range(nt):
                ref[t, x, 0:PAD, :] = edge
                ref[t, x, PAD + ny:, :] = edge
        return 0

    lax.fori_loop(0, nxp, clear_rows, 0)
    for ref, planes in ((u0, (-2, -1, nx, nx + 1)), (u1, (-3, -2, nx + 1, nx + 2)),
                        (u2, (-4, -3, nx + 2, nx + 3)), (f, (-3, -2, -1, nx, nx + 1, nx + 2))):
        for x in planes:
            for t in range(nt):
                ref[t, x + FX] = jnp.zeros((nyp, LANES), f32)

    def clear_px(i, _):
        for t in range(nt):
            px[t, i, 0:PAD, :] = edge
            px[t, i, PAD + ny:, :] = jnp.zeros((2 * PAD, LANES), f32)
        return 0

    lax.fori_loop(0, mx + 4, clear_px, 0)
    for ref in (e0, e1, e2):
        ref[...] = jnp.zeros(ref.shape, f32)
    for ref in (s1, s2, rs):
        for g in range(tiles):
            ref[g, 0:PAD, :] = edge
            ref[g, PAD + wide:, :] = edge
    pk[...] = jnp.zeros(pk.shape, f32)
    for ref in (c0, c1, c2, c3):
        def clear_c(i, _, ref=ref):
            ref[i, 0:PAD, :] = edge
            ref[i, PAD + rows_c:, :] = edge
            return 0
        lax.fori_loop(0, mx + PAD, clear_c, 0)
    for ref in (d0, d1, d2, d3):
        for g in range(tiles):
            ref[g, 0:PAD, :] = edge
            ref[g, PAD + rows_c:, :] = edge
    for ref in (g0, g1, g2):
        ref[...] = jnp.zeros(ref.shape, f32)
    xe[...] = jnp.zeros(xe.shape, f32)
    for d in NEIGHBOURS:
        refs = []
        if d in PLANAR:
            refs.append(rm.at[PLANAR.index(d)])
        if d[0]:
            refs.append(rpx.at[NEIGHBOURS.index(d)])
        else:
            refs.append(rp.at[(d[1] + 1) * 3 + d[2] + 1])
        if d in SPILL_Z:
            refs.append(spr.at[SPILL_Z.index(d)])
        if d[1:] == (0, 0):
            refs.append(xr.at[int(d[0] > 0)])
        elif d[0] == d[2] == 0:
            refs.append(yr.at[int(d[1] > 0)])
        elif d in PLANAR:
            refs.append(xer.at[[e for e in PLANAR if e[0] and e[1]].index(d)])

        @pl.when(jnp.logical_not(there(minus(d))))
        def _(refs=refs):
            for ref in refs:
                ref[...] = jnp.zeros(ref.shape, f32)

    lane1 = iota((1, LANES), 1)

    def slots(lane, width):
        return lax.rem(lane + width // 2, LANES) // width, lax.rem(lane + width // 2, width) - width // 2

    def zinside(o, reach_low, reach_high):
        low = jnp.logical_and(o >= 0, o < reach_low)
        high = jnp.logical_and(o < 0, o >= -reach_high)
        return jnp.where(low, below[2], jnp.where(high, above[2], 0.0))

    for g in range(tiles):
        shape = (wide, LANES)
        p, o = slots(iota(shape, 1), FINE_SLOT)
        value = inside(g * 16 + p - 8, 0, nx) * inside(iota(shape, 0) - 4, 1, ny)
        fm[g] = value * zinside(o, 3, 3)
        shape = (rows_c, LANES)
        p, o = slots(iota(shape, 1), COARSE_SLOT)
        value = inside(g * 8 + p - 4, 0, mx) * inside(iota(shape, 0) - 4, 1, my)
        em[g] = value * zinside(o, 4, 3)
    kc[...] = inside(iota((rows_c, LANES), 0) - 4, 1, my)

    lane = iota((block, LANES), 1)
    slot, _ = slots(lane, FINE_SLOT)
    first_lane, last_lane = lane == 0, lane == LANES - 1
    low_half = lane < LANES // 2
    inject_1 = jnp.where(low_half, below[2], above[2]) * SMOOTH

    def row_mask(at):
        index = iota((block, LANES), 0) + (at - 4)
        if at == 0 or at + block == wide:
            return inside(index, 1, ny)
        return None

    row_masks = [row_mask(at) for at in blocks]

    def plane_mask(X):
        return inside(X - FX, 0, nx)

    def plane_of(u, X, at):
        return [u[t, X, pl.ds(at + 4, block), :] for t in range(nt)]

    def edges_of(planes):
        return jnp.where(low_half, planes[0], planes[nt - 1])

    def place(X):
        index = X + (8 - FX)
        return divide(index, 16)

    def keep_edges(ref, X, at, planes):
        g, p = place(X)
        pltpu.store(
            ref.at[g, pl.ds(PAD + at, block), :], rotated(edges_of(planes), p * FINE_SLOT), mask=slot == p)


    zero_b = jnp.zeros((block, LANES), f32)

    def across(u, X, at, count, inject_of):
        planes = [plane_of(u, X + n, at) for n in range(-1, count + 1)]
        sums = []
        row = at + 4
        for n in range(count):
            middle = planes[n + 1]
            left = [rotated(p, 1) for p in middle]
            right = [rotated(p, LANES - 1) for p in middle]
            inject = inject_of(X + n)
            one = []
            for t in range(nt):
                before = jnp.where(first_lane, left[t - 1] if t else inject, left[t])
                after = jnp.where(last_lane, right[t + 1] if t < nt - 1 else inject, right[t])
                total = planes[n][t] + planes[n + 2][t]
                total = total + (u[t, X + n, pl.ds(row - 1, block), :] + u[t, X + n, pl.ds(row + 1, block), :])
                total = total + f[t, X + n, pl.ds(row, block), :]
                one.append(total + (before + after))
            sums.append(one)
        return planes[1:-1], sums

    def grouped(first, last, by, body, carry=0):
        count = last - first
        by = max(n for n in range(1, by + 1) if count % n == 0)
        if count == by:
            return body(first, by, carry)
        return lax.fori_loop(0, count // by, lambda j, c: body(first + j * by, by, c), carry)


    def sweep(old, new, X0, X1, keep, before=None):
        for at, mask in zip(blocks, row_masks):
            def step(X, by, _, at=at, mask=mask):
                def inject_of(X):
                    if before is None:
                        return zero_b
                    return edges_of(plane_of(before, X, at)) * inject_1

                planes, sums = across(old, X, at, by, inject_of)
                for n in range(by):
                    factor = SMOOTH * plane_mask(X + n)
                    if mask is not None:
                        factor = factor * mask
                    for t in range(nt):
                        new[t, X + n, pl.ds(at + 4, block), :] = (planes[n][t] + sums[n][t]) * factor
                    keep_edges(keep, X + n, at, planes[n])
                return 0

            grouped(X0, X1, BY, step)

    def sides(ref, g, rows, width, slot_s, off, edge_ref):
        here = ref[g, rows, :]
        count = LANES // width
        zero = jnp.zeros_like(here)
        previous = rotated(ref[g - 1, rows, :], width) if g else zero
        following = rotated(ref[g + 1, rows, :], LANES - width) if g < tiles - 1 else zero
        total = jnp.where(slot_s == 0, previous, rotated(here, width))
        total = total + jnp.where(slot_s == count - 1, following, rotated(here, LANES - width))
        start, length = rows.start, rows.size
        total = total + ref[g, pl.ds(start - 1, length), :] + ref[g, pl.ds(start + 1, length), :]
        touching = edge_ref[g, rows, :]
        total = total + jnp.where(off == 0, touching, rotated(here, 1))
        total = total + jnp.where(off == -1, touching, rotated(here, LANES - 1))
        return here, total

    lane_w = iota((wide, LANES), 1)
    slot_w, off_w = slots(lane_w, FINE_SLOT)
    rows_w = pl.ds(PAD, wide)
    at_edge = jnp.where(jnp.logical_or(off_w == 0, off_w == -1), SMOOTH, 0.0)

    def strips_1(g):
        s1[g, rows_w, :] = e0[g, rows_w, :] * fm[g] * at_edge

    def strips_2(g):
        here, total = sides(s1, g, rows_w, FINE_SLOT, slot_w, off_w, e1)
        s2[g, rows_w, :] = (here + total) * fm[g] * SMOOTH

    def restrict_x(first, last, carries):
        results = []
        for at, mask, carry in zip(blocks, row_masks, carries):
            def step(i, by, part, at=at, mask=mask):
                X = FX + 2 * i - 3
                def inject_of(X):
                    g, p = place(X)
                    return turned_back(s2[g, pl.ds(PAD + at, block), :], p * FINE_SLOT)

                planes, sums = across(u2, X, at, 2 * by, inject_of)
                for n in range(2 * by):
                    keep_edges(e2, X + n, at, planes[n])
                    for t in range(nt):
                        sums[n][t] = sums[n][t] - 6.0 * planes[n][t]
                for n in range(by):
                    half_x, quarter_x = 0.5 * plane_mask(X + 2 * n), 0.25 * plane_mask(X + 2 * n + 1)
                    quarters = [quarter_x * sums[2 * n + 1][t] for t in range(nt)]
                    for t in range(nt):
                        value = part[t] + half_x * sums[2 * n][t] + quarters[t]
                        if mask is not None:
                            value = value * mask
                        px[t, i + n, pl.ds(at + 4, block), :] = value
                    part = quarters
                return part

            results.append(grouped(first, last, BYX, step, carry))
        return results

    flat = u2.reshape(nt, nxp * nyp, LANES)

    def rows_along(y, first, count):
        return pl.ds((FX + first) * nyp + PAD + y, count, stride=nyp)

    corners = [d for d in PLANAR if d[0] and d[1]]

    def row_part(d, first, length):
        if d == 0:
            return pl.ds(first, length)
        return pl.ds(first + (length - PAD if d > 0 else 0), PAD)

    spill_sent, waits_m, waits_p = [], [], []
    last_tile = tiles - 1

    def pack_spill(g):
        here = s2[g, rows_w, :]
        value = jnp.where(off_w == 0, rotated(here, 1), jnp.where(off_w == 1, rotated(here, 3), 0.0))
        value = jnp.where(off_w == -1, rotated(here, LANES - 1), value)
        sp[g, rows_w, :] = jnp.where(off_w == -2, rotated(here, LANES - 3), value)
        low, high = max(0, 16 * g - 8), min(nx, 16 * g + 8)
        for side, y in ((0, -2), (1, ny)):
            for k in range(2):
                for t in range(nt):
                    ys[side, k, t, low:high] = flat[t, rows_along(y + k, low, high - low), :]
        for n, (dx, dy, _) in enumerate(corners):
            if g == (last_tile if dx > 0 else 0):
                X, y = (FX + nx if dx > 0 else FX - 1), (PAD + ny if dy > 0 else PAD - 1)
                for t in range(nt):
                    xe[n, t:t + 1, :] = u2[t, X, y:y + 1, :]

    def send_spill(g):
        low, high = max(0, 16 * g - 8), min(nx, 16 * g + 8)
        planes = pl.ds(low, high - low)
        for n, dy in enumerate((-1, 1)):
            spill_sent.append(send(ys.at[n, :, :, planes, :], yr.at[n, :, :, planes, :], (0, dy, 0)))
        for n, (dx, dy, dz) in enumerate(SPILL_Z):
            if dx:
                if g == (last_tile if dx > 0 else 0):
                    spill_sent.append(send(sp.at[pl.ds(g, 1), rows_w, :], spr.at[n, pl.ds(0, 1)], (dx, dy, dz)))
            elif dy == 0:
                spill_sent.append(send(sp.at[pl.ds(g, 1), rows_w, :], spr.at[n, pl.ds(g, 1)], (dx, dy, dz)))
            elif g in (last_tile - 2, last_tile):
                some = pl.ds(0, g + 1) if g < last_tile else pl.ds(g - 1, 2)
                rows = row_part(dy, PAD, wide)
                spill_sent.append(send(sp.at[some, rows, :], spr.at[n, some, pl.ds(0, PAD), :], (dx, dy, dz)))
        for n, d in enumerate(corners):
            if g == (last_tile if d[0] > 0 else 0):
                spill_sent.append(send(xe.at[n], xer.at[n], d))
        for n, dx in enumerate((-1, 1)):
            if g == (last_tile if dx > 0 else 0):
                source = u2.at[:, pl.ds(FX + nx if dx > 0 else FX - 2, 2), pl.ds(PAD, ny), :]
                spill_sent.append(send(source, xr.at[n], (dx, 0, 0)))

    quarter, half = 0.25 * STEP, 0.5 * STEP

    def step_y(i, _):
        for t in range(nt):
            evens = px[t, i, pl.ds(0, rows_c, stride=2), :]
            odds = px[t, i, pl.ds(1, rows_c, stride=2), :]
            nexts = px[t, i, pl.ds(2, rows_c, stride=2), :]
            py[i, :, t * LANES:(t + 1) * LANES] = quarter * (evens + nexts) + half * odds
        return 0


    def weights(gap, scale):
        outer = jnp.logical_or(gap == 0, gap == 2)
        return jnp.where(gap == 1, 0.5 * scale, jnp.where(outer, 0.25 * scale, 0.0))

    def packed_index(o):
        k = jnp.where(o >= 4, mz + 3 - o, jnp.where(o >= 2, mz - 2 + o, jnp.where(o >= 0, -1 - o, mz - 1 - o)))
        return jnp.where(o <= -7, o + 6, jnp.where(jnp.logical_and(o <= -4, o >= -6), -4 - o, k))

    z_of, n_of = iota((nz, LANES), 0), iota((nz, LANES), 1)
    down = weights(z_of - 2 * n_of, 1.0)
    q_of, o_of = slots(n_of, COARSE_SLOT)
    pack_down = jnp.where(jnp.logical_and(q_of == 0, o_of != -3), weights(z_of - 2 * packed_index(o_of), 1.0), 0.0)
    down = jnp.concatenate([down, pack_down], 1).astype(jnp.bfloat16)
    k_of, n_of = iota((2 * LANES, LANES), 0), iota((2 * LANES, LANES), 1)
    over = k_of >= LANES
    p_of, of_of = slots(jnp.where(over, k_of - LANES, k_of), FINE_SLOT)
    p_of = jnp.where(over, p_of + 16, p_of)
    zf_of = jnp.where(of_of >= 0, -1 - of_of, nz - 1 - of_of)
    q_of, o_of = slots(n_of, COARSE_SLOT)
    kk_of = jnp.where(o_of == -3, mz - 1, packed_index(o_of))
    used = jnp.logical_and(of_of != 3, of_of != -4)
    pack_strip = weights(p_of - 2 * q_of, 1.0) * weights(zf_of - 2 * kk_of, 1.0)
    pack_strip = jnp.where(used, pack_strip, 0.0).astype(jnp.bfloat16)

    lane_c = iota((rows_c, LANES), 1)
    slot_c, off_c = slots(lane_c, COARSE_SLOT)
    rows_m = pl.ds(PAD, rows_c)

    def place_c(index):
        return divide(index, 8)

    pack = 4 if (mx + 4) % 4 == 0 else 1

    def step_z(j, _):
        both = split_dot(py[pl.ds(j * pack, pack)].reshape(pack * rows_c, nz), down)
        both = both.reshape(pack, rows_c, 2 * LANES)
        for n in range(pack):
            index = j * pack + n + 2
            mp[index, rows_m, :] = both[n, :, :LANES]
            g, q = place_c(index)
            pltpu.store(pk.at[g, rows_m, :], rotated(both[n, :, LANES:], q * COARSE_SLOT), mask=slot_c == q)
        return 0

    def strip_y(g):
        start = SR - 8
        evens = rs[g, pl.ds(start, rows_c, stride=2), :]
        odds = rs[g, pl.ds(start + 1, rows_c, stride=2), :]
        nexts = rs[g, pl.ds(start + 2, rows_c, stride=2), :]
        return quarter * (evens + nexts) + half * odds

    def strips_pack(g):
        beyond = strip_y(g + 1) if g + 1 < tiles else jnp.zeros((rows_c, LANES), f32)
        pk[g, rows_m, :] += split_dot(jnp.concatenate([strip_y(g), beyond], 1), pack_strip)

    def send_planes(first, last):
        for n, d in enumerate(PLANAR):
            rows = row_part(d[1], PAD, rows_c)
            if d[0] == 0:
                planes, target = pl.ds(first, last - first), pl.ds(first - 2, last - first)
            elif (last == mx + 6) if d[0] > 0 else (first == 2):
                planes, target = (pl.ds(mx, 6), pl.ds(0, 6)) if d[0] > 0 else (pl.ds(2, 5), pl.ds(0, 5))
            else:
                continue
            waits_m.append(send(mp.at[planes, rows, :], rm.at[n, target, pl.ds(0, rows.size), :], d))

    def send_strips(first, last):
        final = last == tiles
        for side in range(2):
            for g in range(first, last, 2):
                value = pk[g, rows_m, :]
                if g + 1 < tiles:
                    keep = off_c >= 0 if side else off_c < 0
                    value = jnp.where(keep, value, rotated(pk[g + 1, rows_m, :], -8 if side else 8))
                pz[side, g // 2, rows_m, :] = value
        pairs = pl.ds(first // 2, (last + 1) // 2 - first // 2)
        for n, d in enumerate(NEIGHBOURS):
            rows = row_part(d[1], PAD, rows_c)
            if d[0]:
                if (d[0] > 0) == final:
                    target = rpx.at[n, :, pl.ds(0, rows.size), :]
                    waits_p.append(send(pk.at[pl.ds(last_tile if final else 0, 1), rows, :], target, d))
                continue
            some = pairs if d[2] else pl.ds(first, last - first)
            source = pz.at[int(d[2] > 0), some, rows, :] if d[2] else pk.at[some, rows, :]
            target = rp.at[(d[1] + 1) * 3 + d[2] + 1, some, pl.ds(0, rows.size), :]
            waits_p.append(send(source, target, d))

    carries = [[zero_b] * nt for _ in blocks]

    def restrict_part(first, last, first_g, last_g):
        for g in range(first_g, min(last_g + 1, tiles)):
            here, total = sides(s2, g, rows_w, FINE_SLOT, slot_w, off_w, e2)
            rs[g, rows_w, :] = (total - 6.0 * here) * fm[g]
        unrolled(first, last, step_y, 0, 4)
        unrolled(first // pack, last // pack, step_z, 0, BYP)
        at_first = len(sent)
        send_planes(first + 2, last + 2)
        for g in range(first_g, last_g):
            strips_pack(g)
        send_strips(first_g, last_g)
        start(range(at_first, len(sent)))

    for c in range(chunks):
        for load in loads[c * 2 * nt:(c + 1) * 2 * nt]:
            load.wait()
        final = c == chunks - 1
        low, high = 16 * c, (nx + 1 if final else 16 * c + 15)
        sweep(u0, u1, FX + low - 1, FX + high, e0)
        sweep(u1, u2, FX + low - 2, FX + (high + 1 if final else high - 1), e1, u0)
        strips_1(c)
        strips_1(c + 1)
        for g in range(c, tiles if final else c + 1):
            strips_2(g)
            pack_spill(g)
        if not final:
            if c == 0:
                pl.semaphore_wait(barrier, expected)
            at_first = len(sent)
            send_spill(c)
            start(range(at_first, len(sent)))
        carries = restrict_x(max(0, 8 * c - 3), mx + 3 if final else 8 * c + 5, carries)
        if c == chunks - 2:
            ready = (8 * c + 5) // pack * pack
            whole = (ready + 2) // 16 * 2
            restrict_part(0, ready, 0, whole)
    for at, mask, part in zip(blocks, row_masks, carries):
        for t in range(nt):
            px[t, mx + 3, pl.ds(at + 4, block), :] = part[t] if mask is None else part[t] * mask
    restrict_part(ready, mx + 4, whole, tiles)
    at_first, early = len(sent), len(spill_sent)
    for g in (last_tile - 1, last_tile):
        send_spill(g)
    start(range(at_first, len(sent)))

    lane_n = iota((ny, LANES), 1)
    low_lanes, high_lanes = lane_n < 2, lane_n >= LANES - 2
    at_z = {d: n for n, d in enumerate(SPILL_Z)}
    rest = 16 * last_tile - 24

    def add_spills(late):
        arrive(spill_sent[early:] if late else spill_sent[:early])
        n, X = (1, FX) if late else (0, FX + nx - 2)
        for k in range(2):
            for t in range(nt):
                u2[t, X + k, pl.ds(PAD, ny), :] += xr[n, t, k]
        first, count = (rest, nx - rest) if late else (0, rest)
        for n, y in enumerate((ny - 2, 0)):
            for k in range(2):
                for t in range(nt):
                    flat[t, rows_along(y + k, first, count), :] += yr[n, k, t, first:first + count]
        for n, (dx, dy, _) in enumerate(corners):
            if (dx > 0) == late:
                X, y = (FX if dx > 0 else FX + nx - 1), (PAD if dy > 0 else PAD + ny - 1)
                for t in range(nt):
                    u2[t, X, y:y + 1, :] += xer[n, t:t + 1, :]
        some = (0, last_tile - 1, last_tile) if late else range(1, last_tile - 1)
        for g in some:
            parts = []
            for dz in (1, -1):
                pieces = [spr[at_z[(0, 0, dz)], g]]
                for dx in (-1, 1):
                    if g == (last_tile if dx < 0 else 0):
                        pieces.append(spr[at_z[(dx, 0, dz)], 0])
                part = sum(pieces[1:], pieces[0])
                top = part[0:PAD] + spr[at_z[(0, 1, dz)], g, 0:PAD]
                end = part[wide - PAD:] + spr[at_z[(0, -1, dz)], g, 0:PAD]
                parts.append(jnp.concatenate([top, part[PAD:wide - PAD], end], 0))
            s1[g, rows_w, :] = jnp.where(off_w >= 0, parts[0], parts[1])
            for x in range(max(0, 16 * g - 8), min(nx, 16 * g + 8)):
                p = divide(x + 8, 16)[1]
                value = turned_back(s1[g, pl.ds(SR, ny), :], p * FINE_SLOT)
                u2[0, x + FX, pl.ds(PAD, ny), :] += jnp.where(low_lanes, value, 0.0)
                u2[nt - 1, x + FX, pl.ds(PAD, ny), :] += jnp.where(high_lanes, value, 0.0)

    add_spills(False)

    arrive(waits_m + waits_p)
    at_p = {d: n for n, d in enumerate(NEIGHBOURS)}
    at_m = {d: n for n, d in enumerate(PLANAR)}
    last = rows_c - PAD

    def row_at(dy):
        return 0 if dy > 0 else last

    pieces = {}
    for dz in SIDES:
        for g in range(tiles):
            at = g if dz == 0 else g // 2
            base = pk[g, rows_m, :] if dz == 0 else rp[3 + dz + 1, at]
            parts = [base[r:r + PAD] for r in range(0, rows_c, PAD)]
            for dy in (-1, 1):
                parts[row_at(dy) // PAD] += rp[(dy + 1) * 3 + dz + 1, at, 0:PAD]
            if g in (0, last_tile):
                dx = -1 if g else 1
                for dy in SIDES:
                    ref = rpx.at[at_p[(dx, dy, dz)], 0]
                    if dy == 0:
                        for n in range(rows_c // PAD):
                            parts[n] += ref[n * PAD:(n + 1) * PAD]
                    else:
                        parts[row_at(dy) // PAD] += ref[0:PAD]
            whole_rows = jnp.concatenate(parts, 0)
            pieces[dz, g] = rotated(whole_rows, 8 * dz) if dz and g % 2 else whole_rows
    for g in range(tiles):
        own, low, high = (pieces[dz, g] for dz in (0, 1, -1))
        value = jnp.where(jnp.logical_and(off_c >= -2, off_c <= 1), own, 0.0)
        value = value + jnp.where(off_c >= 0, rotated(low, LANES - 4), rotated(high, 3))
        d0[g, rows_m, :] = value * em[g]
        lowest = jnp.where(jnp.logical_or(off_c == 0, off_c == 1), rotated(low, LANES - 2), 0.0)
        highest = jnp.where(jnp.logical_or(off_c == -1, off_c == -2), rotated(high, 6), 0.0)
        ad[g] = lowest + highest + jnp.where(off_c == -1, rotated(own, 2), 0.0)

    first_c, last_c = lane_c == 0, lane_c == LANES - 1
    near_c = jnp.logical_or(lane_c < 2, lane_c >= LANES - 2)

    def plane_mask_c(index):
        return inside(index - 4, 0, mx)

    def build(index, extra=None):
        g, q = place_c(index)
        here = mp[index, rows_m, :] if extra is None else extra
        value = here + jnp.where(near_c, turned_back(ad[g], q * COARSE_SLOT), 0.0)
        value = value * (kc[...] * plane_mask_c(index))
        c0[index, rows_m, :] = value

    def rows_added(index):
        first = mp[index, pl.ds(PAD, PAD), :] + rm[at_m[(0, 1, 0)], index - 2, 0:PAD]
        middle = mp[index, pl.ds(2 * PAD, rows_c - 2 * PAD), :]
        final = mp[index, pl.ds(PAD + last, PAD), :] + rm[at_m[(0, -1, 0)], index - 2, 0:PAD]
        return jnp.concatenate([first, middle, final], 0)

    def planes_added(dx, k, own):
        value = rm[at_m[(dx, 0, 0)], k] + (own if own is not None else 0.0)
        first = value[0:PAD] + rm[at_m[(dx, 1, 0)], k, 0:PAD]
        final = value[last:] + rm[at_m[(dx, -1, 0)], k, 0:PAD]
        return jnp.concatenate([first, value[PAD:last], final], 0)

    for k in range(6):
        build(k, planes_added(1, k, rows_added(k) if k >= 2 else None))

    def build_inner(index, _):
        build(index, rows_added(index))
        return 0

    unrolled(6, mx + 2, build_inner, 0, BYC)
    for k in range(5):
        index = mx + 2 + k
        build(index, planes_added(-1, k, rows_added(index) if index < mx + 6 else None))

    grids, strips, touch = (c0, c1, c2, c3), (d0, d1, d2, d3), (g0, g1, g2)
    for k in range(COARSE_SWEEPS - 1):
        old, new = grids[k], grids[k + 1]

        def sweep_c(index, _, old=old, new=new, k=k):
            g, q = place_c(index)
            inject = turned_back(strips[k][g, rows_m, :], q * COARSE_SLOT)
            here = old[index, rows_m, :]
            total = here + old[index - 1, rows_m, :] + old[index + 1, rows_m, :]
            total = total + old[index, pl.ds(PAD - 1, rows_c), :] + old[index, pl.ds(PAD + 1, rows_c), :]
            total = total + jnp.where(first_c, inject, rotated(here, 1))
            total = total + jnp.where(last_c, inject, rotated(here, LANES - 1))
            value = total * (kc[...] * (plane_mask_c(index) * (0.25 * STEP))) + c0[index, rows_m, :]
            new[index, rows_m, :] = value
            pltpu.store(touch[k].at[g, rows_m, :], rotated(here, q * COARSE_SLOT), mask=slot_c == q)
            return 0

        unrolled(k + 1, mx + 6 - k, sweep_c, 0, BYC)
        for g in range(tiles):
            here, total = sides(strips[k], g, rows_m, COARSE_SLOT, slot_c, off_c, touch[k])
            strips[k + 1][g, rows_m, :] = (here + total) * (em[g] * (0.25 * STEP)) + d0[g, rows_m, :]

    add_spills(True)

    up = weights(iota((mz, nz), 1) - 2 * iota((mz, nz), 0), 2.0).astype(jnp.bfloat16)
    three = 3 if (mx + 1) % 3 == 0 else 1

    def prolong_z(j, _):
        value = split_dot(c3[pl.ds(3 + j * three, three), rows_m, :].reshape(three * rows_c, LANES), up)
        for n in range(three):
            g, q = place_c(3 + j * three + n)
            outside = 0.5 * turned_back(d3[g, rows_m, :], q * COARSE_SLOT)
            for t in range(nt):
                part = value[n * rows_c:(n + 1) * rows_c, t * LANES:(t + 1) * LANES]
                if t == 0:
                    part = part + jnp.where(first_c, outside, 0.0)
                q_ref[j * three + n, t] = part
        return 0

    unrolled(0, (mx + 1) // three, prolong_z, 0, 3)

    for d, some in by_direction(range(len(sent))):
        @pl.when(there(d))
        def _(d=d, some=some):
            for number in some:
                sent[number][0](d).wait_send()


def add_kernel(per, smooth_ref, q_ref, out_hbm, both, out_ref, sems):
    mx, nt, my = q_ref.shape[0] - 1, q_ref.shape[1], q_ref.shape[2] - PAD
    ny = 2 * my

    def spread(p, _):
        for t in range(nt):
            here = q_ref[p, t, 4:4 + my, :]
            before = q_ref[p, t, 3:3 + my, :]
            both[p, t, pl.ds(0, my, stride=2), :] = 0.5 * (before + here)
            both[p, t, pl.ds(1, my, stride=2), :] = here
        return 0

    def add(j, _):
        for t in range(nt):
            part = pl.ds(t * LANES, LANES)
            here = both[j + 1, t]
            first = smooth_ref[t, 2 * j + FX, PAD:PAD + ny, :]
            second = smooth_ref[t, 2 * j + FX + 1, PAD:PAD + ny, :]
            out_ref[2 * j, :, part] = first + 0.5 * (both[j, t] + here)
            out_ref[2 * j + 1, :, part] = second + here
        return 0

    copies = []
    spread(0, 0)
    for c in range(mx // per):
        lax.fori_loop(c * per + 1, (c + 1) * per + 1, spread, 0, unroll=2)
        lax.fori_loop(c * per, (c + 1) * per, add, 0)
        rows = pl.ds(2 * c * per, 2 * per)
        copies.append(pltpu.make_async_copy(out_ref.at[rows], out_hbm.at[rows], sems.at[c]))
        copies[-1].start()
    for copy in copies:
        copy.wait()


def on_device(sizes, start_field, right_side):
    nx, ny, nz = start_field.shape
    nt, mx, my = nz // LANES, nx // 2, ny // 2
    tiles = (nx + 16) // 16
    f32 = jnp.float32

    def vm(*shape):
        return pltpu.VMEM(shape, f32)

    fine_shape = (nt, nx + 2 * FX, ny + 2 * PAD, LANES)
    fine = vm(*fine_shape)
    strip = vm(tiles, ny + 3 * PAD, LANES)
    strip_c = vm(tiles, my + 3 * PAD, LANES)
    coarse = vm(mx + PAD, my + 3 * PAD, LANES)
    vmem = pl.BlockSpec(memory_space=pltpu.VMEM)
    smooth, q = pl.pallas_call(
        functools.partial(correct_kernel, sizes),
        out_shape=(
            pltpu.VMEM(fine_shape, f32),
            pltpu.VMEM((mx + 1, nt, my + PAD, LANES), f32),
        ),
        in_specs=[pl.BlockSpec(memory_space=pltpu.HBM)] * 2,
        out_specs=(vmem, vmem),
        scratch_shapes=[
            fine, fine, fine,
            vm(nt, mx + 4, ny + 3 * PAD, LANES), vm(mx + 4, my + PAD, nz),
            strip, strip, strip, strip, strip, strip,
            strip, vm(len(SPILL_Z), tiles, ny + PAD, LANES), vm(tiles, ny + PAD, LANES),
            vm(2, 2, nt, nx, LANES), vm(2, 2, nt, nx, LANES), vm(2, nt, 2, ny, LANES), vm(4, PAD, LANES), vm(4, PAD, LANES),
            coarse, strip_c, vm(2, (tiles + 1) // 2, my + 3 * PAD, LANES),
            vm(tiles, my + PAD, LANES), vm(my + PAD, LANES),
            vm(len(PLANAR), mx + 4, my + PAD, LANES), vm(9, tiles, my + PAD, LANES),
            vm(len(NEIGHBOURS), 1, my + PAD, LANES),
            coarse, coarse, coarse, coarse, strip_c, strip_c, strip_c, strip_c, strip_c, strip_c, strip_c,
            vm(tiles, my + PAD, LANES),
            pltpu.SemaphoreType.DMA((2 * nt * tiles,)),
            pltpu.SemaphoreType.DMA((N_COPIES,)),
            pltpu.SemaphoreType.DMA((N_COPIES,)),
        ],
        compiler_params=pltpu.CompilerParams(
            collective_id=0, has_side_effects=True, vmem_limit_bytes=48 * 1024 * 1024),
    )(*(pltpu.with_memory_space_constraint(a, pltpu.HBM) for a in (start_field, right_side)))
    per = 8 if mx % 8 == 0 else 1
    return pl.pallas_call(
        functools.partial(add_kernel, per),
        out_shape=jax.ShapeDtypeStruct((nx, ny, nz), f32),
        in_specs=[vmem, vmem],
        out_specs=pl.BlockSpec(memory_space=pl.ANY),
        scratch_shapes=[
            pltpu.VMEM((mx + 1, nt, ny, LANES), f32), pltpu.VMEM((nx, ny, nz), f32),
            pltpu.SemaphoreType.DMA((mx // per,)),
        ],
        compiler_params=pltpu.CompilerParams(vmem_limit_bytes=24 * 1024 * 1024),
    )(smooth, q)


def solution(mesh):
    placed = (P(*AXES), P(*AXES))
    sizes = tuple(mesh.shape[a] for a in AXES)
    return jax.shard_map(
        functools.partial(on_device, sizes), mesh=mesh, in_specs=placed, out_specs=P(*AXES), check_vma=False
    )
```

```python
import functools

import jax
import jax.numpy as jnp
from jax import lax
from jax.experimental import pallas as pl
from jax.experimental.pallas import tpu as pltpu
from jax.sharding import PartitionSpec as P

OMEGA = 6.0 / 7.0
SMOOTH = 1.0 - OMEGA
STEP = OMEGA / 1.5
COARSE_SWEEPS = 4
BY = 20
BYX = 14
BYC = 40
BYP = 5
BYZ = 8
LANES = 128
PAD = 8
FX = 4
FINE_SLOT = 8
COARSE_SLOT = 16
SR = 12
AXES = ("gx", "gy", "gz")
MESH = pl.DeviceIdType.MESH
SIDES = (-1, 0, 1)
NEIGHBOURS = tuple((x, y, z) for x in SIDES for y in SIDES for z in SIDES if (x, y, z) != (0, 0, 0))
PLANAR = tuple(d for d in NEIGHBOURS if d[2] == 0)
SPILL_Z = tuple(d for d in NEIGHBOURS if d[2] and not (d[0] and d[1]))
N_COPIES = 160


def rotated(values, shift):
    if isinstance(shift, int) and shift % LANES == 0:
        return values
    return pltpu.roll(values, shift % LANES if isinstance(shift, int) else shift, values.ndim - 1)


def split_dot(values, matrix):
    high = values.astype(jnp.bfloat16)
    rest = values - high.astype(jnp.float32)
    middle = rest.astype(jnp.bfloat16)
    low = (rest - middle.astype(jnp.float32)).astype(jnp.bfloat16)
    total = jnp.dot(low, matrix, preferred_element_type=jnp.float32)
    total = total + jnp.dot(middle, matrix, preferred_element_type=jnp.float32)
    return total + jnp.dot(high, matrix, preferred_element_type=jnp.float32)


def divide(index, by):
    if isinstance(index, int):
        return divmod(index, by)
    return lax.div(index, by), lax.rem(index, by)


def turned_back(values, shift):
    if isinstance(shift, int):
        return rotated(values, -shift)
    return rotated(values, lax.rem(LANES - shift, LANES))


def unrolled(first, last, body, carry, by):
    count = (last - first) // by

    def several(j, carry):
        for n in range(by):
            carry = body(first + j * by + n, carry)
        return carry

    if count:
        carry = lax.fori_loop(0, count, several, carry)
    for index in range(first + count * by, last):
        carry = body(index, carry)
    return carry


def fine_block(ny):
    rows = ny + PAD
    return 24 if rows % 24 == 0 else 8


def correct_kernel(
    sizes, start_hbm, right_hbm, u2, q_ref,
    u0, u1, f, px, py, e0, e1, e2, s1, s2, rs, sp, spr, fm,
    ys, yr, xr, xe, xer,
    mp, pk, pz, em, kc, rm, rp, rpx, c0, c1, c2, c3, d0, d1, d2, d3, g0, g1, g2, ad,
    local_sem, send_sem, recv_sem,
):
    nt, nxp, nyp, _ = f.shape
    nx, ny = nxp - 2 * FX, nyp - 2 * PAD
    nz = nt * LANES
    mx, my, mz = nx // 2, ny // 2, nz // 2
    tiles = fm.shape[0]
    wide = ny + PAD
    block = fine_block(ny)
    blocks = range(0, wide, block)
    rows_c = my + PAD
    me = tuple(lax.axis_index(a) for a in AXES)
    f32 = jnp.float32

    def there(d):
        found = None
        for at, step, size in zip(me, d, sizes):
            if step:
                one = at < size - 1 if step > 0 else at > 0
                found = one if found is None else jnp.logical_and(found, one)
        return found

    def minus(d):
        return tuple(-c for c in d)

    def device(d):
        return tuple(at + step for at, step in zip(me, d))

    sent = []

    def by_direction(numbers):
        found = {}
        for number in numbers:
            found.setdefault(sent[number][1], []).append(number)
        return found.items()

    def send(src, dst, d):
        number = len(sent)

        def copy(to):
            return pltpu.make_async_remote_copy(
                src_ref=src, dst_ref=dst, send_sem=send_sem.at[number],
                recv_sem=recv_sem.at[number], device_id=device(to), device_id_type=MESH)

        sent.append((copy, d))
        return number

    def start(numbers):
        for d, some in by_direction(numbers):
            @pl.when(there(d))
            def _(d=d, some=some):
                for number in some:
                    sent[number][0](d).start()

    def arrive(numbers):
        for d, some in by_direction(numbers):
            @pl.when(there(minus(d)))
            def _(d=d, some=some):
                for number in some:
                    sent[number][0](minus(d)).wait_recv()

    def iota(shape, axis):
        return lax.broadcasted_iota(jnp.int32, shape, axis)

    chunks = tiles - 1
    bounds = [16 * c for c in range(tiles)]
    loads = []
    for low, high in zip(bounds[:-1], bounds[1:]):
        for into, source in ((u0, start_hbm), (f, right_hbm)):
            for t in range(nt):
                load = pltpu.make_async_copy(
                    source.at[pl.ds(low, high - low), :, pl.ds(t * LANES, LANES)],
                    into.at[t, pl.ds(FX + low, high - low), pl.ds(PAD, ny), :], local_sem.at[len(loads)])
                load.start()
                loads.append(load)

    barrier = pltpu.get_barrier_semaphore()
    expected = jnp.int32(0)
    for d in NEIGHBOURS:
        @pl.when(there(d))
        def _(d=d):
            pl.semaphore_signal(barrier, inc=1, device_id=device(d), device_id_type=MESH)
        expected = expected + there(d).astype(jnp.int32)

    def ones(flag):
        return jnp.where(flag, 1.0, 0.0).astype(f32)

    below = tuple(ones(at > 0) for at in me)
    above = tuple(ones(at < size - 1) for at, size in zip(me, sizes))

    def inside(index, axis, length):
        if isinstance(index, int):
            return below[axis] if index < 0 else above[axis] if index >= length else 1.0
        return jnp.where(index < 0, below[axis], jnp.where(index >= length, above[axis], 1.0))

    edge = jnp.zeros((PAD, LANES), f32)

    def clear_rows(x, _):
        for ref in (u0, u1, u2, f):
            for t in range(nt):
                ref[t, x, 0:PAD, :] = edge
                ref[t, x, PAD + ny:, :] = edge
        return 0

    lax.fori_loop(0, nxp, clear_rows, 0)
    for ref, planes in ((u0, (-2, -1, nx, nx + 1)), (u1, (-3, -2, nx + 1, nx + 2)),
                        (u2, (-4, -3, nx + 2, nx + 3)), (f, (-3, -2, -1, nx, nx + 1, nx + 2))):
        for x in planes:
            for t in range(nt):
                ref[t, x + FX] = jnp.zeros((nyp, LANES), f32)

    def clear_px(i, _):
        for t in range(nt):
            px[t, i, 0:PAD, :] = edge
            px[t, i, PAD + ny:, :] = jnp.zeros((2 * PAD, LANES), f32)
        return 0

    lax.fori_loop(0, mx + 4, clear_px, 0)
    for ref in (e0, e1, e2):
        ref[...] = jnp.zeros(ref.shape, f32)
    for ref in (s1, s2, rs):
        for g in range(tiles):
            ref[g, 0:PAD, :] = edge
            ref[g, PAD + wide:, :] = edge
    pk[...] = jnp.zeros(pk.shape, f32)
    for ref in (c0, c1, c2, c3):
        def clear_c(i, _, ref=ref):
            ref[i, 0:PAD, :] = edge
            ref[i, PAD + rows_c:, :] = edge
            return 0
        lax.fori_loop(0, mx + PAD, clear_c, 0)
    for ref in (d0, d1, d2, d3):
        for g in range(tiles):
            ref[g, 0:PAD, :] = edge
            ref[g, PAD + rows_c:, :] = edge
    for ref in (g0, g1, g2):
        ref[...] = jnp.zeros(ref.shape, f32)
    xe[...] = jnp.zeros(xe.shape, f32)
    for d in NEIGHBOURS:
        refs = []
        if d in PLANAR:
            refs.append(rm.at[PLANAR.index(d)])
        if d[0]:
            refs.append(rpx.at[NEIGHBOURS.index(d)])
        else:
            refs.append(rp.at[(d[1] + 1) * 3 + d[2] + 1])
        if d in SPILL_Z:
            refs.append(spr.at[SPILL_Z.index(d)])
        if d[1:] == (0, 0):
            refs.append(xr.at[int(d[0] > 0)])
        elif d[0] == d[2] == 0:
            refs.append(yr.at[int(d[1] > 0)])
        elif d in PLANAR:
            refs.append(xer.at[[e for e in PLANAR if e[0] and e[1]].index(d)])

        @pl.when(jnp.logical_not(there(minus(d))))
        def _(refs=refs):
            for ref in refs:
                ref[...] = jnp.zeros(ref.shape, f32)

    lane1 = iota((1, LANES), 1)

    def slots(lane, width):
        return lax.rem(lane + width // 2, LANES) // width, lax.rem(lane + width // 2, width) - width // 2

    def zinside(o, reach_low, reach_high):
        low = jnp.logical_and(o >= 0, o < reach_low)
        high = jnp.logical_and(o < 0, o >= -reach_high)
        return jnp.where(low, below[2], jnp.where(high, above[2], 0.0))

    for g in range(tiles):
        shape = (wide, LANES)
        p, o = slots(iota(shape, 1), FINE_SLOT)
        value = inside(g * 16 + p - 8, 0, nx) * inside(iota(shape, 0) - 4, 1, ny)
        fm[g] = value * zinside(o, 3, 3)
        shape = (rows_c, LANES)
        p, o = slots(iota(shape, 1), COARSE_SLOT)
        value = inside(g * 8 + p - 4, 0, mx) * inside(iota(shape, 0) - 4, 1, my)
        em[g] = value * zinside(o, 4, 3)
    kc[...] = inside(iota((rows_c, LANES), 0) - 4, 1, my)

    lane = iota((block, LANES), 1)
    slot, _ = slots(lane, FINE_SLOT)
    first_lane, last_lane = lane == 0, lane == LANES - 1
    low_half = lane < LANES // 2
    inject_1 = jnp.where(low_half, below[2], above[2]) * SMOOTH

    def row_mask(at):
        index = iota((block, LANES), 0) + (at - 4)
        if at == 0 or at + block == wide:
            return inside(index, 1, ny)
        return None

    row_masks = [row_mask(at) for at in blocks]

    def plane_mask(X):
        return inside(X - FX, 0, nx)

    def plane_of(u, X, at):
        return [u[t, X, pl.ds(at + 4, block), :] for t in range(nt)]

    def edges_of(planes):
        return jnp.where(low_half, planes[0], planes[nt - 1])

    def place(X):
        index = X + (8 - FX)
        return divide(index, 16)

    def keep_edges(ref, X, at, planes):
        g, p = place(X)
        pltpu.store(
            ref.at[g, pl.ds(PAD + at, block), :], rotated(edges_of(planes), p * FINE_SLOT), mask=slot == p)


    zero_b = jnp.zeros((block, LANES), f32)

    def across(u, X, at, count, inject_of):
        planes = [plane_of(u, X + n, at) for n in range(-1, count + 1)]
        sums = []
        row = at + 4
        for n in range(count):
            middle = planes[n + 1]
            left = [rotated(p, 1) for p in middle]
            right = [rotated(p, LANES - 1) for p in middle]
            inject = inject_of(X + n)
            one = []
            for t in range(nt):
                before = jnp.where(first_lane, left[t - 1] if t else inject, left[t])
                after = jnp.where(last_lane, right[t + 1] if t < nt - 1 else inject, right[t])
                total = planes[n][t] + planes[n + 2][t]
                total = total + (u[t, X + n, pl.ds(row - 1, block), :] + u[t, X + n, pl.ds(row + 1, block), :])
                total = total + f[t, X + n, pl.ds(row, block), :]
                one.append(total + (before + after))
            sums.append(one)
        return planes[1:-1], sums

    def grouped(first, last, by, body, carry=0):
        count = last - first
        by = max(n for n in range(1, by + 1) if count % n == 0)
        if count == by:
            return body(first, by, carry)
        return lax.fori_loop(0, count // by, lambda j, c: body(first + j * by, by, c), carry)


    def sweep(old, new, X0, X1, keep, before=None):
        for at, mask in zip(blocks, row_masks):
            def step(X, by, _, at=at, mask=mask):
                def inject_of(X):
                    if before is None:
                        return zero_b
                    return edges_of(plane_of(before, X, at)) * inject_1

                planes, sums = across(old, X, at, by, inject_of)
                for n in range(by):
                    factor = SMOOTH * plane_mask(X + n)
                    if mask is not None:
                        factor = factor * mask
                    for t in range(nt):
                        new[t, X + n, pl.ds(at + 4, block), :] = (planes[n][t] + sums[n][t]) * factor
                    keep_edges(keep, X + n, at, planes[n])
                return 0

            grouped(X0, X1, BY, step)

    def sides(ref, g, rows, width, slot_s, off, edge_ref):
        here = ref[g, rows, :]
        count = LANES // width
        zero = jnp.zeros_like(here)
        previous = rotated(ref[g - 1, rows, :], width) if g else zero
        following = rotated(ref[g + 1, rows, :], LANES - width) if g < tiles - 1 else zero
        total = jnp.where(slot_s == 0, previous, rotated(here, width))
        total = total + jnp.where(slot_s == count - 1, following, rotated(here, LANES - width))
        start, length = rows.start, rows.size
        total = total + ref[g, pl.ds(start - 1, length), :] + ref[g, pl.ds(start + 1, length), :]
        touching = edge_ref[g, rows, :]
        total = total + jnp.where(off == 0, touching, rotated(here, 1))
        total = total + jnp.where(off == -1, touching, rotated(here, LANES - 1))
        return here, total

    lane_w = iota((wide, LANES), 1)
    slot_w, off_w = slots(lane_w, FINE_SLOT)
    rows_w = pl.ds(PAD, wide)
    at_edge = jnp.where(jnp.logical_or(off_w == 0, off_w == -1), SMOOTH, 0.0)

    def strips_1(g):
        s1[g, rows_w, :] = e0[g, rows_w, :] * fm[g] * at_edge

    def strips_2(g):
        here, total = sides(s1, g, rows_w, FINE_SLOT, slot_w, off_w, e1)
        s2[g, rows_w, :] = (here + total) * fm[g] * SMOOTH

    def restrict_x(first, last, carries):
        results = []
        for at, mask, carry in zip(blocks, row_masks, carries):
            def step(i, by, part, at=at, mask=mask):
                X = FX + 2 * i - 3
                def inject_of(X):
                    g, p = place(X)
                    return turned_back(s2[g, pl.ds(PAD + at, block), :], p * FINE_SLOT)

                planes, sums = across(u2, X, at, 2 * by, inject_of)
                for n in range(2 * by):
                    keep_edges(e2, X + n, at, planes[n])
                    for t in range(nt):
                        sums[n][t] = sums[n][t] - 6.0 * planes[n][t]
                for n in range(by):
                    half_x, quarter_x = 0.5 * plane_mask(X + 2 * n), 0.25 * plane_mask(X + 2 * n + 1)
                    quarters = [quarter_x * sums[2 * n + 1][t] for t in range(nt)]
                    for t in range(nt):
                        value = part[t] + half_x * sums[2 * n][t] + quarters[t]
                        if mask is not None:
                            value = value * mask
                        px[t, i + n, pl.ds(at + 4, block), :] = value
                    part = quarters
                return part

            results.append(grouped(first, last, BYX, step, carry))
        return results

    flat = u2.reshape(nt, nxp * nyp, LANES)

    def rows_along(y, first, count):
        return pl.ds((FX + first) * nyp + PAD + y, count, stride=nyp)

    corners = [d for d in PLANAR if d[0] and d[1]]

    def row_part(d, first, length):
        if d == 0:
            return pl.ds(first, length)
        return pl.ds(first + (length - PAD if d > 0 else 0), PAD)

    spill_sent, waits_m, waits_p = [], [], []
    last_tile = tiles - 1

    def pack_spill(g):
        here = s2[g, rows_w, :]
        value = jnp.where(off_w == 0, rotated(here, 1), jnp.where(off_w == 1, rotated(here, 3), 0.0))
        value = jnp.where(off_w == -1, rotated(here, LANES - 1), value)
        sp[g, rows_w, :] = jnp.where(off_w == -2, rotated(here, LANES - 3), value)
        low, high = max(0, 16 * g - 8), min(nx, 16 * g + 8)
        for side, y in ((0, -2), (1, ny)):
            for k in range(2):
                for t in range(nt):
                    ys[side, k, t, low:high] = flat[t, rows_along(y + k, low, high - low), :]
        for n, (dx, dy, _) in enumerate(corners):
            if g == (last_tile if dx > 0 else 0):
                X, y = (FX + nx if dx > 0 else FX - 1), (PAD + ny if dy > 0 else PAD - 1)
                for t in range(nt):
                    xe[n, t:t + 1, :] = u2[t, X, y:y + 1, :]

    def send_spill(g):
        low, high = max(0, 16 * g - 8), min(nx, 16 * g + 8)
        planes = pl.ds(low, high - low)
        for n, dy in enumerate((-1, 1)):
            spill_sent.append(send(ys.at[n, :, :, planes, :], yr.at[n, :, :, planes, :], (0, dy, 0)))
        for n, (dx, dy, dz) in enumerate(SPILL_Z):
            if dx:
                if g == (last_tile if dx > 0 else 0):
                    spill_sent.append(send(sp.at[pl.ds(g, 1), rows_w, :], spr.at[n, pl.ds(0, 1)], (dx, dy, dz)))
            elif dy == 0:
                spill_sent.append(send(sp.at[pl.ds(g, 1), rows_w, :], spr.at[n, pl.ds(g, 1)], (dx, dy, dz)))
            elif g in (last_tile - 2, last_tile):
                some = pl.ds(0, g + 1) if g < last_tile else pl.ds(g - 1, 2)
                rows = row_part(dy, PAD, wide)
                spill_sent.append(send(sp.at[some, rows, :], spr.at[n, some, pl.ds(0, PAD), :], (dx, dy, dz)))
        for n, d in enumerate(corners):
            if g == (last_tile if d[0] > 0 else 0):
                spill_sent.append(send(xe.at[n], xer.at[n], d))
        for n, dx in enumerate((-1, 1)):
            if g == (last_tile if dx > 0 else 0):
                source = u2.at[:, pl.ds(FX + nx if dx > 0 else FX - 2, 2), pl.ds(PAD, ny), :]
                spill_sent.append(send(source, xr.at[n], (dx, 0, 0)))

    quarter, half = 0.25 * STEP, 0.5 * STEP

    def step_y(i, _):
        for t in range(nt):
            evens = px[t, i, pl.ds(0, rows_c, stride=2), :]
            odds = px[t, i, pl.ds(1, rows_c, stride=2), :]
            nexts = px[t, i, pl.ds(2, rows_c, stride=2), :]
            py[i, :, t * LANES:(t + 1) * LANES] = quarter * (evens + nexts) + half * odds
        return 0


    def weights(gap, scale):
        outer = jnp.logical_or(gap == 0, gap == 2)
        return jnp.where(gap == 1, 0.5 * scale, jnp.where(outer, 0.25 * scale, 0.0))

    def packed_index(o):
        k = jnp.where(o >= 4, mz + 3 - o, jnp.where(o >= 2, mz - 2 + o, jnp.where(o >= 0, -1 - o, mz - 1 - o)))
        return jnp.where(o <= -7, o + 6, jnp.where(jnp.logical_and(o <= -4, o >= -6), -4 - o, k))

    z_of, n_of = iota((nz, LANES), 0), iota((nz, LANES), 1)
    down = weights(z_of - 2 * n_of, 1.0)
    q_of, o_of = slots(n_of, COARSE_SLOT)
    pack_down = jnp.where(jnp.logical_and(q_of == 0, o_of != -3), weights(z_of - 2 * packed_index(o_of), 1.0), 0.0)
    down = jnp.concatenate([down, pack_down], 1).astype(jnp.bfloat16)
    k_of, n_of = iota((2 * LANES, LANES), 0), iota((2 * LANES, LANES), 1)
    over = k_of >= LANES
    p_of, of_of = slots(jnp.where(over, k_of - LANES, k_of), FINE_SLOT)
    p_of = jnp.where(over, p_of + 16, p_of)
    zf_of = jnp.where(of_of >= 0, -1 - of_of, nz - 1 - of_of)
    q_of, o_of = slots(n_of, COARSE_SLOT)
    kk_of = jnp.where(o_of == -3, mz - 1, packed_index(o_of))
    used = jnp.logical_and(of_of != 3, of_of != -4)
    pack_strip = weights(p_of - 2 * q_of, 1.0) * weights(zf_of - 2 * kk_of, 1.0)
    pack_strip = jnp.where(used, pack_strip, 0.0).astype(jnp.bfloat16)

    lane_c = iota((rows_c, LANES), 1)
    slot_c, off_c = slots(lane_c, COARSE_SLOT)
    rows_m = pl.ds(PAD, rows_c)

    def place_c(index):
        return divide(index, 8)

    pack = 4 if (mx + 4) % 4 == 0 else 1

    def step_z(j, _):
        both = split_dot(py[pl.ds(j * pack, pack)].reshape(pack * rows_c, nz), down)
        both = both.reshape(pack, rows_c, 2 * LANES)
        for n in range(pack):
            index = j * pack + n + 2
            mp[index, rows_m, :] = both[n, :, :LANES]
            g, q = place_c(index)
            pltpu.store(pk.at[g, rows_m, :], rotated(both[n, :, LANES:], q * COARSE_SLOT), mask=slot_c == q)
        return 0

    def strip_y(g):
        start = SR - 8
        evens = rs[g, pl.ds(start, rows_c, stride=2), :]
        odds = rs[g, pl.ds(start + 1, rows_c, stride=2), :]
        nexts = rs[g, pl.ds(start + 2, rows_c, stride=2), :]
        return quarter * (evens + nexts) + half * odds

    def strips_pack(g):
        beyond = strip_y(g + 1) if g + 1 < tiles else jnp.zeros((rows_c, LANES), f32)
        pk[g, rows_m, :] += split_dot(jnp.concatenate([strip_y(g), beyond], 1), pack_strip)

    def send_planes(first, last):
        for n, d in enumerate(PLANAR):
            rows = row_part(d[1], PAD, rows_c)
            if d[0] == 0:
                planes, target = pl.ds(first, last - first), pl.ds(first - 2, last - first)
            elif (last == mx + 6) if d[0] > 0 else (first == 2):
                planes, target = (pl.ds(mx, 6), pl.ds(0, 6)) if d[0] > 0 else (pl.ds(2, 5), pl.ds(0, 5))
            else:
                continue
            waits_m.append(send(mp.at[planes, rows, :], rm.at[n, target, pl.ds(0, rows.size), :], d))

    def send_strips(first, last):
        final = last == tiles
        for side in range(2):
            for g in range(first, last, 2):
                value = pk[g, rows_m, :]
                if g + 1 < tiles:
                    keep = off_c >= 0 if side else off_c < 0
                    value = jnp.where(keep, value, rotated(pk[g + 1, rows_m, :], -8 if side else 8))
                pz[side, g // 2, rows_m, :] = value
        pairs = pl.ds(first // 2, (last + 1) // 2 - first // 2)
        for n, d in enumerate(NEIGHBOURS):
            rows = row_part(d[1], PAD, rows_c)
            if d[0]:
                if (d[0] > 0) == final:
                    target = rpx.at[n, :, pl.ds(0, rows.size), :]
                    waits_p.append(send(pk.at[pl.ds(last_tile if final else 0, 1), rows, :], target, d))
                continue
            some = pairs if d[2] else pl.ds(first, last - first)
            source = pz.at[int(d[2] > 0), some, rows, :] if d[2] else pk.at[some, rows, :]
            target = rp.at[(d[1] + 1) * 3 + d[2] + 1, some, pl.ds(0, rows.size), :]
            waits_p.append(send(source, target, d))

    carries = [[zero_b] * nt for _ in blocks]

    def restrict_part(first, last, first_g, last_g):
        for g in range(first_g, min(last_g + 1, tiles)):
            here, total = sides(s2, g, rows_w, FINE_SLOT, slot_w, off_w, e2)
            rs[g, rows_w, :] = (total - 6.0 * here) * fm[g]
        unrolled(first, last, step_y, 0, 4)
        unrolled(first // pack, last // pack, step_z, 0, BYP)
        at_first = len(sent)
        send_planes(first + 2, last + 2)
        for g in range(first_g, last_g):
            strips_pack(g)
        send_strips(first_g, last_g)
        start(range(at_first, len(sent)))

    for c in range(chunks):
        for load in loads[c * 2 * nt:(c + 1) * 2 * nt]:
            load.wait()
        final = c == chunks - 1
        low, high = 16 * c, (nx + 1 if final else 16 * c + 15)
        sweep(u0, u1, FX + low - 1, FX + high, e0)
        sweep(u1, u2, FX + low - 2, FX + (high + 1 if final else high - 1), e1, u0)
        strips_1(c)
        strips_1(c + 1)
        for g in range(c, tiles if final else c + 1):
            strips_2(g)
            pack_spill(g)
        if c == 0:
            pl.semaphore_wait(barrier, expected)
        at_first = len(sent)
        if final:
            early = len(spill_sent)
        for g in range(c, tiles if final else c + 1):
            send_spill(g)
        start(range(at_first, len(sent)))
        carries = restrict_x(max(0, 8 * c - 3), mx + 3 if final else 8 * c + 5, carries)
        if c == chunks - 2:
            ready = (8 * c + 5) // pack * pack
            whole = (ready + 2) // 16 * 2
            restrict_part(0, ready, 0, whole)
    for at, mask, part in zip(blocks, row_masks, carries):
        for t in range(nt):
            px[t, mx + 3, pl.ds(at + 4, block), :] = part[t] if mask is None else part[t] * mask
    restrict_part(ready, mx + 4, whole, tiles)
    lane_n = iota((ny, LANES), 1)
    low_lanes, high_lanes = lane_n < 2, lane_n >= LANES - 2
    at_z = {d: n for n, d in enumerate(SPILL_Z)}
    rest = 16 * last_tile - 24

    def add_spills(late):
        arrive(spill_sent[early:] if late else spill_sent[:early])
        n, X = (1, FX) if late else (0, FX + nx - 2)
        for k in range(2):
            for t in range(nt):
                u2[t, X + k, pl.ds(PAD, ny), :] += xr[n, t, k]
        first, count = (rest, nx - rest) if late else (0, rest)
        for n, y in enumerate((ny - 2, 0)):
            for k in range(2):
                for t in range(nt):
                    flat[t, rows_along(y + k, first, count), :] += yr[n, k, t, first:first + count]
        for n, (dx, dy, _) in enumerate(corners):
            if (dx > 0) == late:
                X, y = (FX if dx > 0 else FX + nx - 1), (PAD if dy > 0 else PAD + ny - 1)
                for t in range(nt):
                    u2[t, X, y:y + 1, :] += xer[n, t:t + 1, :]
        some = (0, last_tile - 1, last_tile) if late else range(1, last_tile - 1)
        for g in some:
            parts = []
            for dz in (1, -1):
                pieces = [spr[at_z[(0, 0, dz)], g]]
                for dx in (-1, 1):
                    if g == (last_tile if dx < 0 else 0):
                        pieces.append(spr[at_z[(dx, 0, dz)], 0])
                part = sum(pieces[1:], pieces[0])
                top = part[0:PAD] + spr[at_z[(0, 1, dz)], g, 0:PAD]
                end = part[wide - PAD:] + spr[at_z[(0, -1, dz)], g, 0:PAD]
                parts.append(jnp.concatenate([top, part[PAD:wide - PAD], end], 0))
            s1[g, rows_w, :] = jnp.where(off_w >= 0, parts[0], parts[1])
            for x in range(max(0, 16 * g - 8), min(nx, 16 * g + 8)):
                p = divide(x + 8, 16)[1]
                value = turned_back(s1[g, pl.ds(SR, ny), :], p * FINE_SLOT)
                u2[0, x + FX, pl.ds(PAD, ny), :] += jnp.where(low_lanes, value, 0.0)
                u2[nt - 1, x + FX, pl.ds(PAD, ny), :] += jnp.where(high_lanes, value, 0.0)

    add_spills(False)
    add_spills(True)

    arrive(waits_m + waits_p)
    at_p = {d: n for n, d in enumerate(NEIGHBOURS)}
    at_m = {d: n for n, d in enumerate(PLANAR)}
    last = rows_c - PAD

    def row_at(dy):
        return 0 if dy > 0 else last

    pieces = {}
    for dz in SIDES:
        for g in range(tiles):
            at = g if dz == 0 else g // 2
            base = pk[g, rows_m, :] if dz == 0 else rp[3 + dz + 1, at]
            parts = [base[r:r + PAD] for r in range(0, rows_c, PAD)]
            for dy in (-1, 1):
                parts[row_at(dy) // PAD] += rp[(dy + 1) * 3 + dz + 1, at, 0:PAD]
            if g in (0, last_tile):
                dx = -1 if g else 1
                for dy in SIDES:
                    ref = rpx.at[at_p[(dx, dy, dz)], 0]
                    if dy == 0:
                        for n in range(rows_c // PAD):
                            parts[n] += ref[n * PAD:(n + 1) * PAD]
                    else:
                        parts[row_at(dy) // PAD] += ref[0:PAD]
            whole_rows = jnp.concatenate(parts, 0)
            pieces[dz, g] = rotated(whole_rows, 8 * dz) if dz and g % 2 else whole_rows
    for g in range(tiles):
        own, low, high = (pieces[dz, g] for dz in (0, 1, -1))
        value = jnp.where(jnp.logical_and(off_c >= -2, off_c <= 1), own, 0.0)
        value = value + jnp.where(off_c >= 0, rotated(low, LANES - 4), rotated(high, 3))
        d0[g, rows_m, :] = value * em[g]
        lowest = jnp.where(jnp.logical_or(off_c == 0, off_c == 1), rotated(low, LANES - 2), 0.0)
        highest = jnp.where(jnp.logical_or(off_c == -1, off_c == -2), rotated(high, 6), 0.0)
        ad[g] = lowest + highest + jnp.where(off_c == -1, rotated(own, 2), 0.0)

    first_c, last_c = lane_c == 0, lane_c == LANES - 1
    near_c = jnp.logical_or(lane_c < 2, lane_c >= LANES - 2)

    def plane_mask_c(index):
        return inside(index - 4, 0, mx)

    def build(index, extra=None):
        g, q = place_c(index)
        here = mp[index, rows_m, :] if extra is None else extra
        value = here + jnp.where(near_c, turned_back(ad[g], q * COARSE_SLOT), 0.0)
        value = value * (kc[...] * plane_mask_c(index))
        c0[index, rows_m, :] = value

    def rows_added(index):
        first = mp[index, pl.ds(PAD, PAD), :] + rm[at_m[(0, 1, 0)], index - 2, 0:PAD]
        middle = mp[index, pl.ds(2 * PAD, rows_c - 2 * PAD), :]
        final = mp[index, pl.ds(PAD + last, PAD), :] + rm[at_m[(0, -1, 0)], index - 2, 0:PAD]
        return jnp.concatenate([first, middle, final], 0)

    def planes_added(dx, k, own):
        value = rm[at_m[(dx, 0, 0)], k] + (own if own is not None else 0.0)
        first = value[0:PAD] + rm[at_m[(dx, 1, 0)], k, 0:PAD]
        final = value[last:] + rm[at_m[(dx, -1, 0)], k, 0:PAD]
        return jnp.concatenate([first, value[PAD:last], final], 0)

    for k in range(6):
        build(k, planes_added(1, k, rows_added(k) if k >= 2 else None))

    def build_inner(index, _):
        build(index, rows_added(index))
        return 0

    unrolled(6, mx + 2, build_inner, 0, BYC)
    for k in range(5):
        index = mx + 2 + k
        build(index, planes_added(-1, k, rows_added(index) if index < mx + 6 else None))

    grids, strips, touch = (c0, c1, c2, c3), (d0, d1, d2, d3), (g0, g1, g2)
    for k in range(COARSE_SWEEPS - 1):
        old, new = grids[k], grids[k + 1]

        def sweep_c(index, _, old=old, new=new, k=k):
            g, q = place_c(index)
            inject = turned_back(strips[k][g, rows_m, :], q * COARSE_SLOT)
            here = old[index, rows_m, :]
            total = here + old[index - 1, rows_m, :] + old[index + 1, rows_m, :]
            total = total + old[index, pl.ds(PAD - 1, rows_c), :] + old[index, pl.ds(PAD + 1, rows_c), :]
            total = total + jnp.where(first_c, inject, rotated(here, 1))
            total = total + jnp.where(last_c, inject, rotated(here, LANES - 1))
            value = total * (kc[...] * (plane_mask_c(index) * (0.25 * STEP))) + c0[index, rows_m, :]
            new[index, rows_m, :] = value
            pltpu.store(touch[k].at[g, rows_m, :], rotated(here, q * COARSE_SLOT), mask=slot_c == q)
            return 0

        unrolled(k + 1, mx + 6 - k, sweep_c, 0, BYC)
        for g in range(tiles):
            here, total = sides(strips[k], g, rows_m, COARSE_SLOT, slot_c, off_c, touch[k])
            strips[k + 1][g, rows_m, :] = (here + total) * (em[g] * (0.25 * STEP)) + d0[g, rows_m, :]

    up = weights(iota((mz, nz), 1) - 2 * iota((mz, nz), 0), 2.0).astype(jnp.bfloat16)
    three = 3 if (mx + 1) % 3 == 0 else 1

    def prolong_z(j, _):
        value = split_dot(c3[pl.ds(3 + j * three, three), rows_m, :].reshape(three * rows_c, LANES), up)
        for n in range(three):
            g, q = place_c(3 + j * three + n)
            outside = 0.5 * turned_back(d3[g, rows_m, :], q * COARSE_SLOT)
            for t in range(nt):
                part = value[n * rows_c:(n + 1) * rows_c, t * LANES:(t + 1) * LANES]
                if t == 0:
                    part = part + jnp.where(first_c, outside, 0.0)
                q_ref[j * three + n, t] = part
        return 0

    unrolled(0, (mx + 1) // three, prolong_z, 0, 3)

    for d, some in by_direction(range(len(sent))):
        @pl.when(there(d))
        def _(d=d, some=some):
            for number in some:
                sent[number][0](d).wait_send()


def add_kernel(per, smooth_ref, q_ref, out_hbm, both, out_ref, sems):
    mx, nt, my = q_ref.shape[0] - 1, q_ref.shape[1], q_ref.shape[2] - PAD
    ny = 2 * my

    def spread(p, _):
        for t in range(nt):
            here = q_ref[p, t, 4:4 + my, :]
            before = q_ref[p, t, 3:3 + my, :]
            both[p, t, pl.ds(0, my, stride=2), :] = 0.5 * (before + here)
            both[p, t, pl.ds(1, my, stride=2), :] = here
        return 0

    def add(j, _):
        for t in range(nt):
            part = pl.ds(t * LANES, LANES)
            here = both[j + 1, t]
            first = smooth_ref[t, 2 * j + FX, PAD:PAD + ny, :]
            second = smooth_ref[t, 2 * j + FX + 1, PAD:PAD + ny, :]
            out_ref[2 * j, :, part] = first + 0.5 * (both[j, t] + here)
            out_ref[2 * j + 1, :, part] = second + here
        return 0

    copies = []
    spread(0, 0)
    for c in range(mx // per):
        lax.fori_loop(c * per + 1, (c + 1) * per + 1, spread, 0, unroll=2)
        lax.fori_loop(c * per, (c + 1) * per, add, 0)
        rows = pl.ds(2 * c * per, 2 * per)
        copies.append(pltpu.make_async_copy(out_ref.at[rows], out_hbm.at[rows], sems.at[c]))
        copies[-1].start()
    for copy in copies:
        copy.wait()


def on_device(sizes, start_field, right_side):
    nx, ny, nz = start_field.shape
    nt, mx, my = nz // LANES, nx // 2, ny // 2
    tiles = (nx + 16) // 16
    f32 = jnp.float32

    def vm(*shape):
        return pltpu.VMEM(shape, f32)

    fine_shape = (nt, nx + 2 * FX, ny + 2 * PAD, LANES)
    fine = vm(*fine_shape)
    strip = vm(tiles, ny + 3 * PAD, LANES)
    strip_c = vm(tiles, my + 3 * PAD, LANES)
    coarse = vm(mx + PAD, my + 3 * PAD, LANES)
    vmem = pl.BlockSpec(memory_space=pltpu.VMEM)
    smooth, q = pl.pallas_call(
        functools.partial(correct_kernel, sizes),
        out_shape=(
            pltpu.VMEM(fine_shape, f32),
            pltpu.VMEM((mx + 1, nt, my + PAD, LANES), f32),
        ),
        in_specs=[pl.BlockSpec(memory_space=pltpu.HBM)] * 2,
        out_specs=(vmem, vmem),
        scratch_shapes=[
            fine, fine, fine,
            vm(nt, mx + 4, ny + 3 * PAD, LANES), vm(mx + 4, my + PAD, nz),
            strip, strip, strip, strip, strip, strip,
            strip, vm(len(SPILL_Z), tiles, ny + PAD, LANES), vm(tiles, ny + PAD, LANES),
            vm(2, 2, nt, nx, LANES), vm(2, 2, nt, nx, LANES), vm(2, nt, 2, ny, LANES), vm(4, PAD, LANES), vm(4, PAD, LANES),
            coarse, strip_c, vm(2, (tiles + 1) // 2, my + 3 * PAD, LANES),
            vm(tiles, my + PAD, LANES), vm(my + PAD, LANES),
            vm(len(PLANAR), mx + 4, my + PAD, LANES), vm(9, tiles, my + PAD, LANES),
            vm(len(NEIGHBOURS), 1, my + PAD, LANES),
            coarse, coarse, coarse, coarse, strip_c, strip_c, strip_c, strip_c, strip_c, strip_c, strip_c,
            vm(tiles, my + PAD, LANES),
            pltpu.SemaphoreType.DMA((2 * nt * tiles,)),
            pltpu.SemaphoreType.DMA((N_COPIES,)),
            pltpu.SemaphoreType.DMA((N_COPIES,)),
        ],
        compiler_params=pltpu.CompilerParams(
            collective_id=0, has_side_effects=True, vmem_limit_bytes=48 * 1024 * 1024),
    )(*(pltpu.with_memory_space_constraint(a, pltpu.HBM) for a in (start_field, right_side)))
    per = 8 if mx % 8 == 0 else 1
    return pl.pallas_call(
        functools.partial(add_kernel, per),
        out_shape=jax.ShapeDtypeStruct((nx, ny, nz), f32),
        in_specs=[vmem, vmem],
        out_specs=pl.BlockSpec(memory_space=pl.ANY),
        scratch_shapes=[
            pltpu.VMEM((mx + 1, nt, ny, LANES), f32), pltpu.VMEM((nx, ny, nz), f32),
            pltpu.SemaphoreType.DMA((mx // per,)),
        ],
        compiler_params=pltpu.CompilerParams(vmem_limit_bytes=24 * 1024 * 1024),
    )(smooth, q)


def solution(mesh):
    placed = (P(*AXES), P(*AXES))
    sizes = tuple(mesh.shape[a] for a in AXES)
    return jax.shard_map(
        functools.partial(on_device, sizes), mesh=mesh, in_specs=placed, out_specs=P(*AXES), check_vma=False
    )
```
